32 devices in a mesh: head: 4 (over z), doc: 8 (over y, x, core).
Axes of the slice: x: 2, y: 2, z: 4, core: 2. Of those that a mesh axis runs over, the one named last changes fastest.
Arguments:
- packed_query_rows: bfloat16 [4096, 4096], P(('doc', 'head')), may hold values from -160 to 160
- packed_key_rows: bfloat16 [4096, 1024], P(('doc', 'head')), may hold values from -6 to 6
- packed_value_rows: bfloat16 [4096, 1024], P(('doc', 'head')), may hold values from -6 to 6
- doc_lengths: int32 [16], replicated, may hold values from 1 to 2048, 4096 in all
Outputs:
- attended: bfloat16 [4096, 4096], P(('doc', 'head'))
The draws below stay inside these ranges and needn't reach their ends.
Inputs may be any that keep to these rules, and one draw needn't show every extreme that they name: `doc_lengths`: the documents lie end to end in order and their lengths sum to 4096.
All inputs are finite; a program needn't handle non-finite values.
Results may differ from the reference program's by a relative error of at most 0.011.
Values may be sent and summed in bfloat16 or wider, within the bound.
No kernel may reach another device: no remote copies, remote signals or barrier semaphores. Data moves between devices by JAX's collectives and lax.ppermute only.
A program may use at most 64 MiB of HBM per device.

```python
import math
import jax
import jax.numpy as jnp
import numpy as np
from jax import lax

QUERY_HEADS = 32
KEY_VALUE_HEADS = 8
HEAD_SIZE = 128
SEG = 512
SEQUENCE_TOKENS = 4096
DOCUMENT_LIMIT = 2048
DOCS = 16
N_DOC = 8


def drawn(key):
    document_sequences = jax.random.split(jax.random.fold_in(key, 7), 1)
    gathered_keys = jnp.clip(jax.random.normal(document_sequences[0], (SEQUENCE_TOKENS, KEY_VALUE_HEADS * HEAD_SIZE), jnp.float32), -6.0, 6.0)
    gathered_keys = gathered_keys.astype(jnp.bfloat16).astype(jnp.float32)
    return gathered_keys


def draw_packed_key_rows(key, part):
    gathered_keys = drawn(key)
    return gathered_keys.astype(jnp.bfloat16)


def draw_packed_query_rows(key, part):
    fresh_key = jax.random.fold_in(key, 13)
    query_tensor = jnp.clip(2.5 * jax.random.normal(fresh_key, (SEQUENCE_TOKENS, QUERY_HEADS * HEAD_SIZE), jnp.float32), -15.0, 15.0)
    return jnp.clip(query_tensor, -160.0, 160.0).astype(jnp.bfloat16)


def steps_of(rng, extent, cuts, least, high):
    level = 1.0
    for position, parts in cuts:
        heights = jax.random.uniform(jax.random.fold_in(jax.random.fold_in(rng, 6), position), (parts,), jnp.float32, least / len(cuts), high / len(cuts))
        level = level * jnp.repeat(jnp.exp(heights), extent[position] // parts).reshape((-1,) + (1,) * (len(extent) - 1 - position))
    return level


def length_profile(count, total, limit, skew):
    portions = [(1 << 20) // math.isqrt(grade ** skew) + 1 for grade in range(2, count + 1)]
    rest, counts = total - limit - (count - 1), [1] * (count - 1)
    while rest > 0:
        free = [i for i in range(count - 1) if counts[i] < limit]
        pool, left = sum([portions[i] for i in free]), rest
        for i in free:
            more = min(limit - counts[i], max(1, left * portions[i] // pool), rest)
            counts[i] = counts[i] + more
            rest = rest - more
    return np.array([limit] + counts)


def ragged(rng, amount, total, reach, lean):
    if amount == 2:
        one = jax.random.randint(rng, (), max(1, total - reach), min(reach, total - 1) + 1)
        return jnp.stack([one, total - one])
    tallies = jnp.asarray(length_profile(amount, total, reach, lean), jnp.int32)
    couples = (amount - 1) // 2
    donor, receiver = tallies[1:1 + 2 * couples:2], tallies[2:2 + 2 * couples:2]
    slack = jnp.minimum(donor - 1, reach - receiver)
    moved = jax.random.randint(jax.random.fold_in(rng, 1), (couples,), 0, 1 << 20) % (slack + 1)
    tallies = tallies.at[1:1 + 2 * couples:2].set(donor - moved).at[2:2 + 2 * couples:2].set(receiver + moved)
    return tallies[jax.random.permutation(jax.random.fold_in(rng, 2), amount)]


def noise(rng, dims, deviation, bound, shards=(), kind=jnp.bfloat16):
    entries = deviation * jax.random.normal(rng, dims, jnp.float32)
    if shards:
        entries = entries * steps_of(rng, dims, shards, -0.22, 0.18)
    return jnp.clip(entries, -bound, bound).astype(kind)


def setup_inputs(seed: int = 0) -> dict:
    key_of = jax.random.split(jax.random.key(seed), 5)
    return {
        "packed_query_rows": draw_packed_query_rows(jax.random.fold_in(key_of[4], 71), 0),
        "packed_key_rows": draw_packed_key_rows(jax.random.fold_in(key_of[4], 71), 0),
        "packed_value_rows": noise(key_of[2], (SEQUENCE_TOKENS, KEY_VALUE_HEADS * HEAD_SIZE), 1.0, 6.0, ((0, 32),)),
        "doc_lengths": ragged(key_of[3], DOCS, SEQUENCE_TOKENS, DOCUMENT_LIMIT, 2).astype(jnp.int32),
    }


NEGATIVE = -1e+30

def doc_starts(doc_lengths, positions):
    closing = jnp.cumsum(doc_lengths)
    passed = closing[None, :] <= positions[:, None]
    return lax.optimization_barrier(jnp.sum(jnp.where(passed, doc_lengths[None, :], 0), axis=1)).astype(jnp.int32)

def reference(packed_query_rows, packed_key_rows, packed_value_rows, doc_lengths):
    group_outputs = QUERY_HEADS // KEY_VALUE_HEADS
    factor = 1.0 / math.sqrt(HEAD_SIZE)
    query_tensor = packed_query_rows.reshape(SEQUENCE_TOKENS, KEY_VALUE_HEADS, group_outputs, HEAD_SIZE)
    filler_length = jnp.zeros((DOCUMENT_LIMIT, KEY_VALUE_HEADS * HEAD_SIZE), packed_key_rows.dtype)
    filled_key_rows = jnp.concatenate([filler_length, packed_key_rows], axis=0).reshape(DOCUMENT_LIMIT + SEQUENCE_TOKENS, KEY_VALUE_HEADS, HEAD_SIZE)
    filled_value_rows = jnp.concatenate([filler_length, packed_value_rows], axis=0).reshape(DOCUMENT_LIMIT + SEQUENCE_TOKENS, KEY_VALUE_HEADS, HEAD_SIZE)
    firsts = doc_starts(doc_lengths, jnp.arange(SEQUENCE_TOKENS, dtype=jnp.int32))

    def one_block(block_index):
        root = (block_index * SEG).astype(jnp.int32)
        block_queries = lax.dynamic_slice_in_dim(query_tensor, root, SEG, 0).astype(jnp.float32)
        block_keys = lax.dynamic_slice_in_dim(filled_key_rows, root, DOCUMENT_LIMIT + SEG, 0).astype(jnp.float32)
        block_values = lax.dynamic_slice_in_dim(filled_value_rows, root, DOCUMENT_LIMIT + SEG, 0).astype(jnp.float32)
        positions = root + jnp.arange(SEG, dtype=jnp.int32)
        key_positions = root - DOCUMENT_LIMIT + jnp.arange(DOCUMENT_LIMIT + SEG, dtype=jnp.int32)
        block_first = lax.dynamic_slice_in_dim(firsts, root, SEG, 0)
        visible = (key_positions[None, :] >= block_first[:, None]) & (key_positions[None, :] <= positions[:, None])

        def single_head(group_member):
            head_queries = lax.dynamic_index_in_dim(block_queries, group_member, 1, keepdims=False)
            head_keys = lax.dynamic_index_in_dim(block_keys, group_member, 1, keepdims=False)
            head_values = lax.dynamic_index_in_dim(block_values, group_member, 1, keepdims=False)
            scores = jnp.einsum('qgd,kd->gqk', head_queries, head_keys) * factor
            scores = jnp.where(visible[None], scores, NEGATIVE)
            highest = lax.optimization_barrier(jnp.max(scores, axis=2, keepdims=True))
            weights = jnp.where(visible[None], jnp.exp(scores - highest), 0.0)
            totals = lax.optimization_barrier(jnp.sum(weights, axis=2))
            rounded = lax.optimization_barrier(weights.astype(jnp.bfloat16)).astype(jnp.float32)
            summed = jnp.einsum('gqk,kd->qgd', rounded, head_values)
            return summed / totals.T[:, :, None]
        head_outputs = lax.map(single_head, jnp.arange(KEY_VALUE_HEADS, dtype=jnp.int32))
        return head_outputs.transpose(1, 0, 2, 3).reshape(SEG, QUERY_HEADS * HEAD_SIZE).astype(jnp.bfloat16)
    blocks = lax.map(one_block, jnp.arange(N_DOC, dtype=jnp.int32))
    return blocks.reshape(SEQUENCE_TOKENS, QUERY_HEADS * HEAD_SIZE)
```

```python
import functools
import math

import jax
import jax.numpy as jnp
from jax import lax
from jax.experimental import pallas as pl
from jax.experimental.pallas import tpu as pltpu
from jax.sharding import PartitionSpec as P

QUERY_HEADS = 32
KEY_VALUE_HEADS = 8
HEAD_SIZE = 128
NEGATIVE = -1e30


def attend_kernel(parts, halo, place_ref, lengths_ref, q_ref, *refs):
    near, far = refs[:parts], refs[parts : parts + halo]
    out_ref, acc_ref, max_ref, sum_ref = refs[parts + halo :]
    width, rows, columns = q_ref.shape
    heads = columns // HEAD_SIZE
    shard = parts * rows
    depth = place_ref[0]
    member = place_ref[1]
    group = place_ref[2]
    scale = math.log2(math.e) / math.sqrt(HEAD_SIZE)

    def one_block(slot, _):
        doc = jnp.bitwise_xor(member, slot)
        root = ((group * width + doc) * parts + depth) * rows
        at = root + lax.broadcasted_iota(jnp.int32, (1, rows), 1)

        def add_doc(i, carry):
            closing, low, high, firsts = carry
            length = lengths_ref[i]
            closing = closing + length
            low = low + jnp.where(closing <= root, length, 0)
            high = high + jnp.where(closing <= root + rows - 1, length, 0)
            firsts = firsts + jnp.where(closing <= at, length, 0)
            return closing, low, high, firsts

        zero = jnp.int32(0)
        _, low, high, firsts = lax.fori_loop(
            0, lengths_ref.shape[0], add_doc, (zero, zero, zero, jnp.zeros((1, rows), jnp.int32))
        )
        q_block = q_ref[slot]
        queries = jnp.concatenate(
            [q_block[:, h * HEAD_SIZE : (h + 1) * HEAD_SIZE] for h in range(heads)], axis=0
        )

        def absorb(source, key_doc, base, masked, opening):
            where = jnp.bitwise_xor(member, key_doc)
            keys = jnp.concatenate([ref[where, :, 0:HEAD_SIZE] for ref in source], axis=0)
            values = jnp.concatenate([ref[where, :, HEAD_SIZE:] for ref in source], axis=0)
            scores = lax.dot_general(
                keys, queries, (((1,), (1,)), ((), ())), preferred_element_type=jnp.float32
            )
            if masked:
                pieces = []
                for s in range(parts):
                    behind = depth - s
                    behind = jnp.where(behind < 0, behind + parts, behind)
                    spot = base + behind * rows + lax.broadcasted_iota(jnp.int32, (rows, rows), 0)
                    seen = (spot >= firsts) & (spot <= at)
                    pieces.append(jnp.concatenate([seen] * heads, axis=1))
                scores = jnp.where(jnp.concatenate(pieces, axis=0), scores, NEGATIVE)
            peak = jnp.max(scores, axis=0, keepdims=True)
            if not opening:
                before = max_ref[...]
                peak = jnp.maximum(before, peak)
            weights = jnp.exp2((scores - peak) * scale)
            total = jnp.sum(weights, axis=0, keepdims=True)
            gain = lax.dot_general(
                values,
                weights.astype(jnp.bfloat16),
                (((0,), (0,)), ((), ())),
                preferred_element_type=jnp.float32,
            )
            if opening:
                sum_ref[...] = total
                acc_ref[...] = gain
            else:
                shrink = jnp.exp2((before - peak) * scale)
                sum_ref[...] = sum_ref[...] * shrink + total
                acc_ref[...] = acc_ref[...] * shrink + gain
            max_ref[...] = peak

        own = (group * width + doc) * shard
        absorb(near, doc, own, True, True)
        lowest = lax.div(low, shard) - group * width

        def earlier(key_doc, _):
            base = (group * width + key_doc) * shard
            clear = base >= high

            def visit(source, index):
                @pl.when(clear)
                def _():
                    absorb(source, index, base, False, False)

                @pl.when(jnp.logical_not(clear))
                def _():
                    absorb(source, index, base, True, False)

            if halo:
                @pl.when(key_doc < 0)
                def _():
                    visit(far, key_doc + width)

                @pl.when(key_doc >= 0)
                def _():
                    visit(near, key_doc)
            else:
                visit(near, key_doc)
            return 0

        lax.fori_loop(lowest, doc, earlier, 0)
        done = acc_ref[...] / sum_ref[...]
        for h in range(heads):
            out_ref[slot, :, h * HEAD_SIZE : (h + 1) * HEAD_SIZE] = (
                done[:, h * rows : (h + 1) * rows].T.astype(out_ref.dtype)
            )
        return 0

    lax.fori_loop(0, width, one_block, 0)


def attend(place, doc_lengths, queries, near, far):
    width, rows, columns = queries.shape
    lanes = columns // HEAD_SIZE * rows
    vmem = pl.BlockSpec(memory_space=pltpu.VMEM)
    smem = pl.BlockSpec(memory_space=pltpu.SMEM)
    return pl.pallas_call(
        functools.partial(attend_kernel, len(near), len(far)),
        out_shape=jax.ShapeDtypeStruct(queries.shape, queries.dtype),
        in_specs=[smem, smem] + [vmem] * (1 + len(near) + len(far)),
        out_specs=vmem,
        scratch_shapes=[
            pltpu.VMEM((HEAD_SIZE, lanes), jnp.float32),
            pltpu.VMEM((1, lanes), jnp.float32),
            pltpu.VMEM((1, lanes), jnp.float32),
        ],
    )(place, doc_lengths, queries, *near, *far)


def exchange(blocks, width):
    length = lax.axis_size("doc")
    return [
        block if k == 0 else lax.ppermute(block, "doc", [(i, i ^ k) for i in range(length)])
        for k, block in enumerate(blocks)
    ]


def on_device(packed_query_rows, packed_key_rows, packed_value_rows, doc_lengths):
    width = KEY_VALUE_HEADS
    docs, parts = lax.axis_size("doc"), lax.axis_size("head")
    index = lax.axis_index("doc")
    member, group = index % width, index // width
    place = jnp.stack([lax.axis_index("head"), member, group]).astype(jnp.int32)

    def cut(value, k):
        size = value.shape[1] // width
        return lax.dynamic_slice_in_dim(value, jnp.bitwise_xor(member, k) * size, size, 1)

    pairs = [
        jnp.concatenate([cut(packed_key_rows, k), cut(packed_value_rows, k)], axis=1)
        for k in range(width)
    ]
    unit = jnp.stack(exchange(pairs, width))
    queries = jnp.stack(exchange([cut(packed_query_rows, k) for k in range(width)], width))
    near = [unit]
    for _ in range(1, parts):
        near.append(
            lax.ppermute(near[-1], "head", [(i, (i + 1) % parts) for i in range(parts)])
        )
    far = []
    if docs > width:
        far = [
            lax.ppermute(piece, "doc", [(i, i + width) for i in range(docs - width)])
            for piece in near
        ]
    attended = attend(place, doc_lengths, queries, near, far)
    returned = exchange([attended[k] for k in range(width)], width)
    stacked = jnp.stack(returned)
    order = [jnp.bitwise_xor(member, k) for k in range(width)]
    return jnp.concatenate(
        [lax.dynamic_index_in_dim(stacked, order[k], 0, keepdims=False) for k in range(width)],
        axis=1,
    )


def solution(mesh):
    in_specs = (P(("doc", "head"), None), P(("doc", "head"), None), P(("doc", "head"), None), P())
    out_specs = P(("doc", "head"), None)
    return jax.shard_map(
        on_device, mesh=mesh, in_specs=in_specs, out_specs=out_specs, check_vma=False
    )
```

```python
import functools
import math

import jax
import jax.numpy as jnp
from jax import lax
from jax.experimental import pallas as pl
from jax.experimental.pallas import tpu as pltpu
from jax.sharding import PartitionSpec as P

KEY_VALUE_HEADS = 8
HEAD_SIZE = 128
NEGATIVE = -1e30
HALVES = 2


def attend_kernel(steps, half, back, slots, opening, closing, parts, place_ref, lengths_ref, *refs):
    width = KEY_VALUE_HEADS
    q_refs, refs = refs[:width], refs[width:]
    units, refs = refs[: len(steps)], refs[len(steps) :]
    if not opening:
        acc_in, stat_in = refs[:2]
        refs = refs[2:]
    if closing:
        out_refs, refs = refs[: len(slots)], refs[len(slots) :]
        acc_ref, stat_ref = refs[:2]
    else:
        acc_out, stat_out = refs[:2]
        acc_ref, stat_ref = refs[2:4]
    q_ref = refs[-2]
    q_sem = refs[-1]
    rows, columns = q_refs[0].shape
    heads = columns // HEAD_SIZE
    lanes = heads * rows
    shard = parts * rows
    chunk = width // HALVES
    depth = place_ref[0]
    member = place_ref[1]
    group = place_ref[2]
    scale = math.log2(math.e) / math.sqrt(HEAD_SIZE)
    first_slot = slots[0]

    copies = [
        pltpu.make_async_copy(q_refs[slot], q_ref.at[slot - first_slot], q_sem) for slot in slots
    ]
    for copy in copies:
        copy.start()
    for copy in copies:
        copy.wait()

    def one_block(turn, _):
        slot = first_slot + turn
        doc = jnp.bitwise_xor(member, slot)
        root = ((group * width + doc) * parts + depth) * rows
        at = root + lax.broadcasted_iota(jnp.int32, (1, rows), 1)

        def add_doc(i, carry):
            closed, low, high, firsts = carry
            length = lengths_ref[i]
            closed = closed + length
            low = low + jnp.where(closed <= root, length, 0)
            high = high + jnp.where(closed <= root + rows - 1, length, 0)
            firsts = firsts + jnp.where(closed <= at, length, 0)
            return closed, low, high, firsts

        zero = jnp.int32(0)
        _, low, high, firsts = lax.fori_loop(
            0,
            lengths_ref.shape[0],
            add_doc,
            (zero, zero, zero, jnp.zeros((1, rows), jnp.int32)),
            unroll=8,
        )
        if opening:
            acc_ref[...] = jnp.zeros_like(acc_ref)
            stat_ref[0:1, :] = jnp.full((1, lanes), NEGATIVE, jnp.float32)
            stat_ref[1:2, :] = jnp.zeros((1, lanes), jnp.float32)
        else:
            acc_ref[...] = acc_in[slot]
            stat_ref[...] = stat_in[slot]
        q_block = q_ref[turn]
        queries = jnp.concatenate(
            [q_block[:, h * HEAD_SIZE : (h + 1) * HEAD_SIZE] for h in range(heads)], axis=0
        )

        def absorb(where, base, masked):
            keys = jnp.concatenate([ref[where, :, 0:HEAD_SIZE] for ref in units], axis=0)
            values = jnp.concatenate([ref[where, :, HEAD_SIZE:] for ref in units], axis=0)
            scores = lax.dot_general(
                keys, queries, (((1,), (1,)), ((), ())), preferred_element_type=jnp.float32
            )
            if masked:
                pieces = []
                for step in steps:
                    behind = depth - step
                    behind = jnp.where(behind < 0, behind + parts, behind)
                    spot = base + behind * rows + lax.broadcasted_iota(jnp.int32, (rows, rows), 0)
                    seen = (spot >= firsts) & (spot <= at)
                    pieces.append(jnp.concatenate([seen] * heads, axis=1))
                scores = jnp.where(jnp.concatenate(pieces, axis=0), scores, NEGATIVE)
            before = stat_ref[0:1, :]
            peak = jnp.maximum(before, jnp.max(scores, axis=0, keepdims=True))
            weights = jnp.exp2((scores - peak) * scale)
            total = jnp.sum(weights, axis=0, keepdims=True)
            gain = lax.dot_general(
                values,
                weights.astype(jnp.bfloat16),
                (((0,), (0,)), ((), ())),
                preferred_element_type=jnp.float32,
            )
            shrink = jnp.exp2((before - peak) * scale)
            stat_ref[0:1, :] = peak
            stat_ref[1:2, :] = stat_ref[1:2, :] * shrink + total
            acc_ref[...] = acc_ref[...] * shrink + gain

        origin = group - back
        lowest = lax.div(low, shard) - origin * width
        bottom = jnp.bitwise_xor(lax.div(member, chunk), half) * chunk
        start = jnp.maximum(lowest, bottom)
        stop = jnp.minimum(doc + back * width, bottom + chunk - 1) + 1

        def visit(key_doc, _):
            base = (origin * width + key_doc) * shard
            where = jnp.bitwise_xor(member, key_doc) - half * chunk
            clear = (base >= high) & (key_doc != doc + back * width)

            @pl.when(clear)
            def _():
                absorb(where, base, False)

            @pl.when(jnp.logical_not(clear))
            def _():
                absorb(where, base, True)

            return 0

        lax.fori_loop(start, stop, visit, 0)
        if closing:
            done = acc_ref[...] / stat_ref[1:2, :]
            for i in range(len(slots)):

                @pl.when(turn == i)
                def _():
                    for h in range(heads):
                        out_refs[i][:, h * HEAD_SIZE : (h + 1) * HEAD_SIZE] = (
                            done[:, h * rows : (h + 1) * rows].T.astype(out_refs[i].dtype)
                        )
        else:
            acc_out[slot] = acc_ref[...]
            stat_out[slot] = stat_ref[...]
        return 0

    lax.fori_loop(0, len(slots), one_block, 0)


def attend(place, doc_lengths, queries, units, steps, half, slots, state, closing, parts, back=0):
    width = KEY_VALUE_HEADS
    rows, columns = queries[0].shape
    lanes = columns // HEAD_SIZE * rows
    vmem = pl.BlockSpec(memory_space=pltpu.VMEM)
    smem = pl.BlockSpec(memory_space=pltpu.SMEM)
    hbm = pl.BlockSpec(memory_space=pl.ANY)
    opening = state is None
    held = () if opening else tuple(state)
    tokens = len(steps) * rows
    accs = jax.ShapeDtypeStruct((width, HEAD_SIZE, lanes), jnp.float32)
    stats = jax.ShapeDtypeStruct((width, 8, lanes), jnp.float32)
    if closing:
        out_shape = [jax.ShapeDtypeStruct((rows, columns), queries[0].dtype) for _ in slots]
        aliases = {}
    else:
        out_shape = [accs, stats]
        first = 2 + width + len(steps)
        aliases = {} if opening else {first: 0, first + 1: 1}
    work = len(slots) * 2 * tokens * lanes * HEAD_SIZE * 4
    return pl.pallas_call(
        functools.partial(
            attend_kernel, tuple(steps), half, back, tuple(slots), opening, closing, parts
        ),
        out_shape=out_shape,
        in_specs=[smem, smem] + [hbm] * width + [vmem] * (len(steps) + len(held)),
        out_specs=[vmem] * len(out_shape),
        input_output_aliases=aliases,
        cost_estimate=pl.CostEstimate(
            flops=work, bytes_accessed=4 * width * HEAD_SIZE * lanes, transcendentals=0
        ),
        scratch_shapes=[
            pltpu.VMEM((HEAD_SIZE, lanes), jnp.float32),
            pltpu.VMEM((8, lanes), jnp.float32),
            pltpu.VMEM((len(slots), rows, columns), queries[0].dtype),
            pltpu.SemaphoreType.DMA,
        ],
    )(place, doc_lengths, *queries, *units, *held)


def swap(block, k):
    if k == 0:
        return block
    length = lax.axis_size("doc")
    return lax.ppermute(block, "doc", [(i, i ^ k) for i in range(length)])


def on_device(packed_query_rows, packed_key_rows, packed_value_rows, doc_lengths):
    width = KEY_VALUE_HEADS
    chunk = width // HALVES
    docs, parts = lax.axis_size("doc"), lax.axis_size("head")
    index = lax.axis_index("doc")
    member, group = index % width, index // width
    place = jnp.stack([lax.axis_index("head"), member, group]).astype(jnp.int32)

    def cut(value, k):
        size = value.shape[1] // width
        return lax.dynamic_slice_in_dim(value, jnp.bitwise_xor(member, k) * size, size, 1)

    ring = [(i, (i + 1) % parts) for i in range(parts)]
    pairs = [
        swap(jnp.concatenate([cut(packed_key_rows, k), cut(packed_value_rows, k)], axis=1), k)
        for k in range(width)
    ]
    units = []
    for half in range(HALVES):
        units.append([jnp.stack(pairs[half * chunk : (half + 1) * chunk])])
    queries = [swap(cut(packed_query_rows, k), k) for k in range(width)]
    for _ in range(1, parts):
        for half in range(HALVES):
            units[half].append(lax.ppermute(units[half][-1], "head", ring))

    attends = functools.partial(attend, place, doc_lengths, queries)
    everyone = list(range(width))
    early = list(range(parts - 1))
    state = None
    if docs > width:
        over = [(i, i + width) for i in range(docs - width)]
        for half in range(HALVES):
            far = [lax.ppermute(piece, "doc", over) for piece in units[half]]
            state = attends(far, list(range(parts)), half, everyone, state, False, parts, back=1)
    for half in range(HALVES):
        state = attends(units[half][:-1], early, half, everyone, state, False, parts)
    for half in range(HALVES - 1):
        state = attends(units[half][-1:], [parts - 1], half, everyone, state, False, parts)
    half = HALVES - 1
    results = {}
    for turn in reversed(range(HALVES)):
        slots = list(range(turn * chunk, (turn + 1) * chunk))
        outs = attends(units[half][-1:], [parts - 1], half, slots, state, True, parts)
        for slot, out in zip(slots, outs):
            results[slot] = swap(out, slot)
    stacked = jnp.stack([results[k] for k in range(width)])
    order = [jnp.bitwise_xor(member, k) for k in range(width)]
    return jnp.concatenate(
        [lax.dynamic_index_in_dim(stacked, order[k], 0, keepdims=False) for k in range(width)],
        axis=1,
    )


def solution(mesh):
    in_specs = (P(("doc", "head"), None), P(("doc", "head"), None), P(("doc", "head"), None), P())
    out_specs = P(("doc", "head"), None)

    return jax.shard_map(
        on_device, mesh=mesh, in_specs=in_specs, out_specs=out_specs, check_vma=False
    )
```

```python
import functools
import math

import jax
import jax.numpy as jnp
from jax import lax
from jax.experimental import pallas as pl
from jax.experimental.pallas import tpu as pltpu
from jax.sharding import PartitionSpec as P

KEY_VALUE_HEADS = 8
HEAD_SIZE = 128
NEGATIVE = -1e30
HALVES = 2


def attend_kernel(half, back, slots, opening, closing, parts, place_ref, bounds_ref, firsts_ref, *refs):
    width = KEY_VALUE_HEADS
    count = len(slots)
    q_refs, refs = refs[:count], refs[count:]
    units, refs = refs[:parts], refs[parts:]
    if not opening:
        acc_in, stat_in = refs[:2]
        refs = refs[2:]
    if closing:
        out_refs, refs = refs[:count], refs[count:]
        acc_ref, stat_ref, q_ref, out_ref, sem = refs
    else:
        acc_out, stat_out, acc_ref, stat_ref, q_ref = refs
    rows, columns = q_refs[0].shape
    heads = columns // HEAD_SIZE
    lanes = heads * rows
    shard = parts * rows
    chunk = width // HALVES
    depth = place_ref[0]
    member = place_ref[1]
    group = place_ref[2]
    scale = math.log2(math.e) / math.sqrt(HEAD_SIZE)

    for i in range(count):
        for h in range(heads):
            q_ref[i, h * rows : (h + 1) * rows, :] = q_refs[i][:, h * HEAD_SIZE : (h + 1) * HEAD_SIZE]

    def one_block(turn, _):
        slot = slots[0] + turn
        doc = jnp.bitwise_xor(member, slot)
        root = ((group * width + doc) * parts + depth) * rows
        at = root + lax.broadcasted_iota(jnp.int32, (1, rows), 1)
        low = bounds_ref[slot, 0]
        high = bounds_ref[slot, 1]
        if opening:
            acc_ref[...] = jnp.zeros_like(acc_ref)
            stat_ref[0:1, :] = jnp.full((1, lanes), NEGATIVE, jnp.float32)
            stat_ref[1:2, :] = jnp.zeros((1, lanes), jnp.float32)
        else:
            acc_ref[...] = acc_in[slot]
            stat_ref[...] = stat_in[slot]

        def absorb(where, base, masked):
            keys = jnp.concatenate([ref[where, :, 0:HEAD_SIZE] for ref in units], axis=0)
            values = jnp.concatenate([ref[where, :, HEAD_SIZE:] for ref in units], axis=0)
            scores = lax.dot_general(
                keys, q_ref[turn], (((1,), (1,)), ((), ())), preferred_element_type=jnp.float32
            )
            if masked:
                firsts = firsts_ref[pl.ds(slot, 1), :]
                pieces = []
                for step in range(parts):
                    behind = depth - step
                    behind = jnp.where(behind < 0, behind + parts, behind)
                    spot = base + behind * rows + lax.broadcasted_iota(jnp.int32, (rows, rows), 0)
                    seen = (spot >= firsts) & (spot <= at)
                    pieces.append(jnp.concatenate([seen] * heads, axis=1))
                scores = jnp.where(jnp.concatenate(pieces, axis=0), scores, NEGATIVE)
            before = stat_ref[0:1, :]
            peak = jnp.maximum(before, jnp.max(scores, axis=0, keepdims=True))
            weights = jnp.exp2((scores - peak) * scale)
            total = jnp.sum(weights, axis=0, keepdims=True)
            gain = lax.dot_general(
                values,
                weights.astype(jnp.bfloat16),
                (((0,), (0,)), ((), ())),
                preferred_element_type=jnp.float32,
            )
            shrink = jnp.exp2((before - peak) * scale)
            stat_ref[0:1, :] = peak
            stat_ref[1:2, :] = stat_ref[1:2, :] * shrink + total
            acc_ref[...] = acc_ref[...] * shrink + gain

        origin = group - back
        lowest = lax.div(low, shard) - origin * width
        bottom = jnp.bitwise_xor(lax.div(member, chunk), half) * chunk
        start = jnp.maximum(lowest, bottom)
        stop = jnp.minimum(doc + back * width, bottom + chunk - 1) + 1

        def visit(key_doc, _):
            base = (origin * width + key_doc) * shard
            where = jnp.bitwise_xor(member, key_doc) - half * chunk
            clear = (base >= high) & (key_doc != doc + back * width)

            @pl.when(clear)
            def _():
                absorb(where, base, False)

            @pl.when(jnp.logical_not(clear))
            def _():
                absorb(where, base, True)

            return 0

        lax.fori_loop(start, stop, visit, 0)
        if closing:
            done = (acc_ref[...] / stat_ref[1:2, :]).astype(out_ref.dtype)
            for h in range(heads):
                out_ref[turn, :, h * HEAD_SIZE : (h + 1) * HEAD_SIZE] = (
                    done[:, h * rows : (h + 1) * rows].T
                )
        else:
            acc_out[slot] = acc_ref[...]
            stat_out[slot] = stat_ref[...]
        return 0

    lax.fori_loop(0, count, one_block, 0)
    if closing:
        copies = [
            pltpu.make_async_copy(out_ref.at[i], out_refs[i], sem.at[i]) for i in range(count)
        ]
        for copy in copies:
            copy.start()
        for copy in copies:
            copy.wait()


def attend(place, tables, queries, units, half, slots, state, closing, parts, back=0):
    width = KEY_VALUE_HEADS
    bounds, firsts = tables
    rows, columns = queries[0].shape
    lanes = columns // HEAD_SIZE * rows
    vmem = pl.BlockSpec(memory_space=pltpu.VMEM)
    smem = pl.BlockSpec(memory_space=pltpu.SMEM)
    hbm = pl.BlockSpec(memory_space=pltpu.HBM)
    opening = state is None
    held = () if opening else tuple(state)
    count = len(slots)
    scratch = [
        pltpu.VMEM((HEAD_SIZE, lanes), jnp.float32),
        pltpu.VMEM((8, lanes), jnp.float32),
        pltpu.VMEM((count, lanes, HEAD_SIZE), queries[0].dtype),
    ]
    if closing:
        out_shape = [jax.ShapeDtypeStruct((rows, columns), queries[0].dtype) for _ in slots]
        out_specs = [hbm] * count
        aliases = {}
        scratch += [
            pltpu.VMEM((count, rows, columns), queries[0].dtype),
            pltpu.SemaphoreType.DMA((count,)),
        ]
    else:
        out_shape = [
            jax.ShapeDtypeStruct((width, HEAD_SIZE, lanes), jnp.float32),
            jax.ShapeDtypeStruct((width, 8, lanes), jnp.float32),
        ]
        out_specs = [vmem, vmem]
        first = 3 + count + len(units)
        aliases = {} if opening else {first: 0, first + 1: 1}
    work = count * 2 * parts * rows * lanes * HEAD_SIZE * 4
    return pl.pallas_call(
        functools.partial(attend_kernel, half, back, tuple(slots), opening, closing, parts),
        out_shape=out_shape,
        in_specs=[smem, smem] + [vmem] * (1 + count + len(units) + len(held)),
        out_specs=out_specs,
        input_output_aliases=aliases,
        cost_estimate=pl.CostEstimate(
            flops=work, bytes_accessed=4 * width * HEAD_SIZE * lanes, transcendentals=0
        ),
        scratch_shapes=scratch,
    )(place, bounds, firsts, *[queries[slot] for slot in slots], *units, *held)


def doc_starts(doc_lengths, positions):
    closing = jnp.cumsum(doc_lengths)
    passed = closing[None, :] <= positions[:, None]
    return jnp.sum(jnp.where(passed, doc_lengths[None, :], 0), axis=1)


def swap(block, k):
    if k == 0:
        return block
    length = lax.axis_size("doc")
    return lax.ppermute(block, "doc", [(i, i ^ k) for i in range(length)])


def on_device(packed_query_rows, packed_key_rows, packed_value_rows, doc_lengths):
    width = KEY_VALUE_HEADS
    chunk = width // HALVES
    docs, parts = lax.axis_size("doc"), lax.axis_size("head")
    index = lax.axis_index("doc")
    member, group = index % width, index // width
    depth = lax.axis_index("head")
    place = jnp.stack([depth, member, group]).astype(jnp.int32)
    rows = packed_query_rows.shape[0]
    blocks = (group * width + jnp.bitwise_xor(member, jnp.arange(width))) * parts + depth
    spots = blocks[:, None] * rows + jnp.arange(rows)[None, :]
    firsts = doc_starts(doc_lengths, spots.reshape(-1)).reshape(width, rows).astype(jnp.int32)
    tables = (jnp.stack([firsts[:, 0], firsts[:, -1]], axis=1), firsts)

    def cut(value, k):
        size = value.shape[1] // width
        return lax.dynamic_slice_in_dim(value, jnp.bitwise_xor(member, k) * size, size, 1)

    ring = [(i, (i + 1) % parts) for i in range(parts)]
    pairs = [
        swap(jnp.concatenate([cut(packed_key_rows, k), cut(packed_value_rows, k)], axis=1), k)
        for k in range(width)
    ]
    units = []
    for half in range(HALVES):
        units.append([jnp.stack(pairs[half * chunk : (half + 1) * chunk])])
    queries = [swap(cut(packed_query_rows, k), k) for k in range(width)]
    for _ in range(1, parts):
        for half in range(HALVES):
            units[half].append(lax.ppermute(units[half][-1], "head", ring))

    attends = functools.partial(attend, place, tables, queries)
    everyone = list(range(width))
    state = None
    if docs > width:
        over = [(i, i + width) for i in range(docs - width)]
        for half in range(HALVES):
            far = [lax.ppermute(piece, "doc", over) for piece in units[half]]
            state = attends(far, half, everyone, state, False, parts, back=1)
    for half in range(HALVES - 1):
        state = attends(units[half], half, everyone, state, False, parts)
    results = {}
    for turn in reversed(range(HALVES)):
        slots = list(range(turn * chunk, (turn + 1) * chunk))
        outs = attends(units[HALVES - 1], HALVES - 1, slots, state, True, parts)
        for slot, out in zip(slots, outs):
            results[slot] = swap(out, slot)
    stacked = jnp.stack([results[k] for k in range(width)])
    order = [jnp.bitwise_xor(member, k) for k in range(width)]
    return jnp.concatenate(
        [lax.dynamic_index_in_dim(stacked, order[k], 0, keepdims=False) for k in range(width)],
        axis=1,
    )


def solution(mesh):
    in_specs = (P(("doc", "head"), None), P(("doc", "head"), None), P(("doc", "head"), None), P())
    out_specs = P(("doc", "head"), None)

    return jax.shard_map(
        on_device, mesh=mesh, in_specs=in_specs, out_specs=out_specs, check_vma=False
    )
```

```python
import functools
import math

import jax
import jax.numpy as jnp
from jax import lax
from jax.experimental import pallas as pl
from jax.experimental.pallas import tpu as pltpu
from jax.sharding import PartitionSpec as P


KEY_VALUE_HEADS = 8
HEAD_SIZE = 128
NEGATIVE = -1e30
HALVES = 2


def attend_kernel(half, back, slots, opening, closing, parts, place_ref, bounds_ref, firsts_ref, *refs):
    width = KEY_VALUE_HEADS
    count = len(slots)
    q_refs, refs = refs[:count], refs[count:]
    units, refs = refs[:parts], refs[parts:]
    if not opening:
        acc_in, stat_in = refs[:2]
        refs = refs[2:]
    if closing:
        out_refs, refs = refs[:count], refs[count:]
    acc_ref, stat_ref, *refs = refs
    score_ref, peak_ref, q_ref, list_ref = refs
    rows, columns = q_refs[0].shape
    heads = columns // HEAD_SIZE
    lanes = heads * rows
    shard = parts * rows
    chunk = width // HALVES
    depth = place_ref[0]
    member = place_ref[1]
    group = place_ref[2]
    origin = group - back
    scale = math.log2(math.e) / math.sqrt(HEAD_SIZE)
    bottom = jnp.bitwise_xor(lax.div(member, chunk), half) * chunk

    visits = jnp.int32(0)
    for turn, slot in enumerate(slots):
        doc = jnp.bitwise_xor(member, slot) + back * width
        lowest = lax.div(bounds_ref[slot], shard) - origin * width
        start = jnp.maximum(lowest, bottom)
        stop = jnp.maximum(jnp.minimum(doc, bottom + chunk - 1) + 1, start)

        def note(key_doc, place, turn=turn):
            list_ref[0, place] = turn
            list_ref[1, place] = key_doc
            return place + 1

        visits = lax.fori_loop(start, stop, note, visits)

    for i in range(count):
        for h in range(heads):
            q_ref[i, h * rows : (h + 1) * rows, :] = q_refs[i][:, h * HEAD_SIZE : (h + 1) * HEAD_SIZE]
    if opening:
        acc_ref[...] = jnp.zeros_like(acc_ref)
        stat_ref[:, 0:1, :] = jnp.full((count, 1, lanes), NEGATIVE, jnp.float32)
        stat_ref[:, 1:2, :] = jnp.zeros((count, 1, lanes), jnp.float32)
    else:
        acc_ref[...] = acc_in[slots[0] : slots[0] + count]
        stat_ref[...] = stat_in[slots[0] : slots[0] + count]

    def multiply(i):
        turn, key_doc = list_ref[0, i], list_ref[1, i]
        where = jnp.bitwise_xor(member, key_doc) - half * chunk
        keys = jnp.concatenate([ref[where, :, 0:HEAD_SIZE] for ref in units], axis=0)
        return lax.dot_general(
            keys, q_ref[turn], (((1,), (1,)), ((), ())), preferred_element_type=jnp.float32
        )

    def settle(i, scores):
        turn, key_doc = list_ref[0, i], list_ref[1, i]
        slot = slots[0] + turn
        doc = jnp.bitwise_xor(member, slot)
        base = (origin * width + key_doc) * shard
        root = ((group * width + doc) * parts + depth) * rows
        at = root + lax.broadcasted_iota(jnp.int32, (1, rows), 1)
        firsts = firsts_ref[pl.ds(slot, 1), :]
        pieces = []
        for step in range(parts):
            behind = depth - step
            behind = jnp.where(behind < 0, behind + parts, behind)
            spot = lax.broadcasted_iota(jnp.int32, (rows, rows), 0)
            corner = base + behind * rows
            seen = (spot >= firsts - corner) & (spot <= at - corner)
            pieces.append(jnp.concatenate([seen] * heads, axis=1))
        scores = jnp.where(jnp.concatenate(pieces, axis=0), scores, NEGATIVE)
        score_ref[...] = scores
        peak_ref[0:1, :] = jnp.max(scores, axis=0, keepdims=True)

    @pl.when(visits > 0)
    def _():
        settle(0, multiply(0))

        def visit(i, _):
            turn, key_doc = list_ref[0, i], list_ref[1, i]
            where = jnp.bitwise_xor(member, key_doc) - half * chunk
            follow = jnp.minimum(i + 1, visits - 1)
            coming = multiply(follow)
            before = stat_ref[turn, 0:1, :]
            peak = jnp.maximum(before, peak_ref[0:1, :])
            weights = jnp.exp2((score_ref[...] - peak) * scale)
            total = jnp.sum(weights, axis=0, keepdims=True)
            values = jnp.concatenate([ref[where, :, HEAD_SIZE:] for ref in units], axis=0)
            gain = lax.dot_general(
                values,
                weights.astype(jnp.bfloat16),
                (((0,), (0,)), ((), ())),
                preferred_element_type=jnp.float32,
            )
            settle(follow, coming)
            shrink = jnp.exp2((before - peak) * scale)
            stat_ref[turn, 0:1, :] = peak
            stat_ref[turn, 1:2, :] = stat_ref[turn, 1:2, :] * shrink + total
            acc_ref[turn] = acc_ref[turn] * shrink + gain
            return 0

        lax.fori_loop(0, visits, visit, 0)

    if closing:
        for i in range(count):
            done = (acc_ref[i] / stat_ref[i, 1:2, :]).astype(out_refs[i].dtype)
            for h in range(heads):
                out_refs[i][:, h * HEAD_SIZE : (h + 1) * HEAD_SIZE] = done[:, h * rows : (h + 1) * rows].T


def attend(place, tables, queries, units, half, slots, state, closing, parts, back=0):
    width = KEY_VALUE_HEADS
    bounds, firsts = tables
    rows, columns = queries[0].shape
    lanes = columns // HEAD_SIZE * rows
    vmem = pl.BlockSpec(memory_space=pltpu.VMEM)
    smem = pl.BlockSpec(memory_space=pltpu.SMEM)
    opening = state is None
    held = () if opening else tuple(state)
    count = len(slots)
    kept = [
        pltpu.VMEM((width, HEAD_SIZE, lanes), jnp.float32),
        pltpu.VMEM((width, 8, lanes), jnp.float32),
    ]
    scratch = [
        pltpu.VMEM((parts * rows, lanes), jnp.float32),
        pltpu.VMEM((8, lanes), jnp.float32),
        pltpu.VMEM((count, lanes, HEAD_SIZE), queries[0].dtype),
        pltpu.SMEM((2, width * width), jnp.int32),
    ]
    aliases = {}
    if closing:
        out_shape = [pltpu.VMEM((rows, columns), queries[0].dtype) for _ in slots]
        scratch = [
            pltpu.VMEM((count, HEAD_SIZE, lanes), jnp.float32),
            pltpu.VMEM((count, 8, lanes), jnp.float32),
        ] + scratch
    else:
        out_shape = kept
        first = 3 + count + len(units)
        aliases = {} if opening else {first: 0, first + 1: 1}
    work = count * 2 * parts * rows * lanes * HEAD_SIZE * 4
    return pl.pallas_call(
        functools.partial(attend_kernel, half, back, tuple(slots), opening, closing, parts),
        out_shape=out_shape,
        in_specs=[smem, smem] + [vmem] * (1 + count + len(units) + len(held)),
        out_specs=[vmem] * len(out_shape),
        input_output_aliases=aliases,
        cost_estimate=pl.CostEstimate(
            flops=work, bytes_accessed=4 * width * HEAD_SIZE * lanes, transcendentals=0
        ),
        scratch_shapes=scratch,
    )(place, bounds, firsts, *[queries[slot] for slot in slots], *units, *held)


def doc_starts(doc_lengths, positions):
    closing = jnp.cumsum(doc_lengths)
    passed = closing[None, :] <= positions[:, None]
    return jnp.sum(jnp.where(passed, doc_lengths[None, :], 0), axis=1)


def swap(block, k):
    if k == 0:
        return block
    length = lax.axis_size("doc")
    return lax.ppermute(block, "doc", [(i, i ^ k) for i in range(length)])


def on_device(packed_query_rows, packed_key_rows, packed_value_rows, doc_lengths):
    width = KEY_VALUE_HEADS
    chunk = width // HALVES
    docs, parts = lax.axis_size("doc"), lax.axis_size("head")
    index = lax.axis_index("doc")
    member, group = index % width, index // width
    depth = lax.axis_index("head")
    place = jnp.stack([depth, member, group]).astype(jnp.int32)
    rows = packed_query_rows.shape[0]
    blocks = (group * width + jnp.bitwise_xor(member, jnp.arange(width))) * parts + depth
    spots = blocks[:, None] * rows + jnp.arange(rows)[None, :]
    firsts = doc_starts(doc_lengths, spots.reshape(-1)).reshape(width, rows).astype(jnp.int32)
    tables = (firsts[:, 0], firsts)

    def cut(value, k):
        size = value.shape[1] // width
        return lax.dynamic_slice_in_dim(value, jnp.bitwise_xor(member, k) * size, size, 1)

    ring = [(i, (i + 1) % parts) for i in range(parts)]
    pairs = [
        swap(jnp.concatenate([cut(packed_key_rows, k), cut(packed_value_rows, k)], axis=1), k)
        for k in range(width)
    ]
    units = []
    for half in range(HALVES):
        units.append([jnp.stack(pairs[half * chunk : (half + 1) * chunk])])
    queries = [swap(cut(packed_query_rows, k), k) for k in range(width)]
    for _ in range(1, parts):
        for half in range(HALVES):
            units[half].append(lax.ppermute(units[half][-1], "head", ring))

    attends = functools.partial(attend, place, tables, queries)
    everyone = list(range(width))
    state = None
    if docs > width:
        over = [(i, i + width) for i in range(docs - width)]
        for half in range(HALVES):
            far = [lax.ppermute(piece, "doc", over) for piece in units[half]]
            state = attends(far, half, everyone, state, False, parts, back=1)
    for half in range(HALVES - 1):
        state = attends(units[half], half, everyone, state, False, parts)
    results = {}
    for turn in reversed(range(HALVES)):
        slots = list(range(turn * chunk, (turn + 1) * chunk))
        outs = attends(units[HALVES - 1], HALVES - 1, slots, state, True, parts)
        for slot, out in zip(slots, outs):
            results[slot] = swap(out, slot)
    stacked = jnp.stack([results[k] for k in range(width)])
    order = [jnp.bitwise_xor(member, k) for k in range(width)]
    return jnp.concatenate(
        [lax.dynamic_index_in_dim(stacked, order[k], 0, keepdims=False) for k in range(width)],
        axis=1,
    )


def solution(mesh):
    in_specs = (P(("doc", "head"), None), P(("doc", "head"), None), P(("doc", "head"), None), P())
    out_specs = P(("doc", "head"), None)

    return jax.shard_map(
        on_device, mesh=mesh, in_specs=in_specs, out_specs=out_specs, check_vma=False
    )
```

```python
import functools
import math

import jax
import jax.numpy as jnp
from jax import lax
from jax.experimental import pallas as pl
from jax.experimental.pallas import tpu as pltpu
from jax.sharding import PartitionSpec as P


KEY_VALUE_HEADS = 8
HEAD_SIZE = 128
NEGATIVE = -1e30
HALVES = 2


def attend_kernel(
    pieces, half, back, slots, opening, closing, parts, place_ref, bounds_ref, firsts_ref, *refs
):
    width = KEY_VALUE_HEADS
    count = len(slots)
    steps = sorted({step for step, _ in pieces})
    q_refs, refs = refs[:count], refs[count:]
    units, refs = refs[: len(pieces)], refs[len(pieces) :]
    if not opening:
        acc_in, stat_in = refs[:2]
        refs = refs[2:]
    if closing:
        out_refs, refs = refs[:count], refs[count:]
    acc_ref, stat_ref, score_ref, peak_ref, q_ref, kv_ref, list_ref = refs
    rows, columns = q_refs[0].shape
    heads = columns // HEAD_SIZE
    lanes = heads * rows
    shard = parts * rows
    depth = place_ref[0]
    member = place_ref[1]
    group = place_ref[2]
    origin = group - back
    scale = math.log2(math.e) / math.sqrt(HEAD_SIZE)
    if half is None:
        bottom, chunk = 0, width
    else:
        chunk = width // HALVES
        bottom = jnp.bitwise_xor(lax.div(member, chunk), half) * chunk

    visits = jnp.int32(0)
    for turn, slot in enumerate(slots):
        doc = jnp.bitwise_xor(member, slot) + back * width
        lowest = lax.div(bounds_ref[slot], shard) - origin * width
        start = jnp.maximum(lowest, bottom)
        stop = jnp.maximum(jnp.minimum(doc, bottom + chunk - 1) + 1, start)

        def note(key_doc, spot, turn=turn):
            list_ref[0, spot] = turn
            list_ref[1, spot] = key_doc
            return spot + 1

        visits = lax.fori_loop(start, stop, note, visits)

    for (step, first), unit in zip(pieces, units):
        at = steps.index(step) * rows
        kv_ref[first : first + unit.shape[0], at : at + rows, :] = unit[...]
    for i in range(count):
        for h in range(heads):
            q_ref[i, h * rows : (h + 1) * rows, :] = q_refs[i][:, h * HEAD_SIZE : (h + 1) * HEAD_SIZE]
    if opening:
        acc_ref[...] = jnp.zeros_like(acc_ref)
        stat_ref[:, 0:1, :] = jnp.full((count, 1, lanes), NEGATIVE, jnp.float32)
        stat_ref[:, 1:2, :] = jnp.zeros((count, 1, lanes), jnp.float32)
    else:
        acc_ref[...] = acc_in[slots[0] : slots[0] + count]
        stat_ref[...] = stat_in[slots[0] : slots[0] + count]

    def multiply(i):
        turn, key_doc = list_ref[0, i], list_ref[1, i]
        keys = kv_ref[jnp.bitwise_xor(member, key_doc), :, 0:HEAD_SIZE]
        return lax.dot_general(
            keys, q_ref[turn], (((1,), (1,)), ((), ())), preferred_element_type=jnp.float32
        )

    def settle(i, scores):
        turn, key_doc = list_ref[0, i], list_ref[1, i]
        slot = slots[0] + turn
        doc = jnp.bitwise_xor(member, slot)
        base = (origin * width + key_doc) * shard
        root = ((group * width + doc) * parts + depth) * rows
        at = root + lax.broadcasted_iota(jnp.int32, (1, rows), 1)
        firsts = firsts_ref[pl.ds(slot, 1), :]
        seen = []
        for step in steps:
            behind = depth - step
            behind = jnp.where(behind < 0, behind + parts, behind)
            spot = lax.broadcasted_iota(jnp.int32, (rows, rows), 0)
            corner = base + behind * rows
            here = (spot >= firsts - corner) & (spot <= at - corner)
            seen.append(jnp.concatenate([here] * heads, axis=1))
        scores = jnp.where(jnp.concatenate(seen, axis=0), scores, NEGATIVE)
        score_ref[...] = scores
        peak_ref[0:1, :] = jnp.max(scores, axis=0, keepdims=True)

    @pl.when(visits > 0)
    def _():
        settle(0, multiply(0))

        def visit(i, _):
            turn, key_doc = list_ref[0, i], list_ref[1, i]
            follow = jnp.minimum(i + 1, visits - 1)
            coming = multiply(follow)
            before = stat_ref[turn, 0:1, :]
            peak = jnp.maximum(before, peak_ref[0:1, :])
            weights = jnp.exp2((score_ref[...] - peak) * scale)
            total = jnp.sum(weights, axis=0, keepdims=True)
            values = kv_ref[jnp.bitwise_xor(member, key_doc), :, HEAD_SIZE:]
            gain = lax.dot_general(
                values,
                weights.astype(jnp.bfloat16),
                (((0,), (0,)), ((), ())),
                preferred_element_type=jnp.float32,
            )
            settle(follow, coming)
            shrink = jnp.exp2((before - peak) * scale)
            stat_ref[turn, 0:1, :] = peak
            stat_ref[turn, 1:2, :] = stat_ref[turn, 1:2, :] * shrink + total
            acc_ref[turn] = acc_ref[turn] * shrink + gain
            return 0

        lax.fori_loop(0, visits, visit, 0)

    if closing:
        for i in range(count):
            done = (acc_ref[i] / stat_ref[i, 1:2, :]).astype(out_refs[i].dtype)
            for h in range(heads):
                out_refs[i][:, h * HEAD_SIZE : (h + 1) * HEAD_SIZE] = done[:, h * rows : (h + 1) * rows].T


def attend(place, tables, queries, pieces, half, slots, state, closing, parts, back=0):
    width = KEY_VALUE_HEADS
    bounds, firsts = tables
    rows, columns = queries[0].shape
    lanes = columns // HEAD_SIZE * rows
    vmem = pl.BlockSpec(memory_space=pltpu.VMEM)
    smem = pl.BlockSpec(memory_space=pltpu.SMEM)
    opening = state is None
    held = () if opening else [pltpu.with_memory_space_constraint(x, pltpu.VMEM) for x in state]
    count = len(slots)
    tokens = len({step for step, _, _ in pieces}) * rows
    kept = [
        pltpu.VMEM((count, HEAD_SIZE, lanes), jnp.float32),
        pltpu.VMEM((count, 8, lanes), jnp.float32),
    ]
    scratch = [
        pltpu.VMEM((tokens, lanes), jnp.float32),
        pltpu.VMEM((8, lanes), jnp.float32),
        pltpu.VMEM((count, lanes, HEAD_SIZE), queries[0].dtype),
        pltpu.VMEM((width, tokens, 2 * HEAD_SIZE), queries[0].dtype),
        pltpu.SMEM((2, width * width), jnp.int32),
    ]
    aliases = {}
    if closing:
        out_shape = [pltpu.VMEM((rows, columns), queries[0].dtype) for _ in slots]
        scratch = kept + scratch
    else:
        out_shape = kept
        first = 3 + count + len(pieces)
        aliases = {} if opening else {first: 0, first + 1: 1}
    work = count * 2 * tokens * lanes * HEAD_SIZE * 4
    return pl.pallas_call(
        functools.partial(
            attend_kernel,
            tuple((step, first) for step, first, _ in pieces),
            half,
            back,
            tuple(slots),
            opening,
            closing,
            parts,
        ),
        out_shape=out_shape,
        in_specs=[smem, smem] + [vmem] * (1 + count + len(pieces) + len(held)),
        out_specs=[vmem] * len(out_shape),
        input_output_aliases=aliases,
        cost_estimate=pl.CostEstimate(
            flops=work, bytes_accessed=4 * width * HEAD_SIZE * lanes, transcendentals=0
        ),
        scratch_shapes=scratch,
    )(
        place,
        bounds,
        firsts,
        *[queries[slot] for slot in slots],
        *[unit for _, _, unit in pieces],
        *held,
    )


def collect_kernel(place_ref, *refs):
    sem = refs[-1]
    out_ref = refs[-2]
    copies = []
    for k, ref in enumerate(refs[:-2]):
        columns = ref.shape[1]
        at = pl.multiple_of(jnp.bitwise_xor(place_ref[1], k) * columns, columns)
        copies.append(pltpu.make_async_copy(ref, out_ref.at[:, pl.ds(at, columns)], sem.at[k]))
    for copy in copies:
        copy.start()
    for copy in copies:
        copy.wait()


def collect(place, blocks):
    rows, columns = blocks[0].shape
    count = len(blocks)
    return pl.pallas_call(
        collect_kernel,
        out_shape=jax.ShapeDtypeStruct((rows, count * columns), blocks[0].dtype),
        in_specs=[pl.BlockSpec(memory_space=pltpu.SMEM)]
        + [pl.BlockSpec(memory_space=pltpu.VMEM)] * count,
        out_specs=pl.BlockSpec(memory_space=pltpu.HBM),
        scratch_shapes=[pltpu.SemaphoreType.DMA((count,))],
    )(place, *blocks)


def doc_starts(doc_lengths, positions):
    closing = jnp.cumsum(doc_lengths)
    passed = closing[None, :] <= positions[:, None]
    return jnp.sum(jnp.where(passed, doc_lengths[None, :], 0), axis=1)


def swap(block, k):
    if k == 0:
        return block
    length = lax.axis_size("doc")
    return lax.ppermute(block, "doc", [(i, i ^ k) for i in range(length)])


def on_device(packed_query_rows, packed_key_rows, packed_value_rows, doc_lengths):
    width = KEY_VALUE_HEADS
    chunk = width // HALVES
    docs, parts = lax.axis_size("doc"), lax.axis_size("head")
    index = lax.axis_index("doc")
    member, group = index % width, index // width
    depth = lax.axis_index("head")
    place = jnp.stack([depth, member, group]).astype(jnp.int32)
    rows = packed_query_rows.shape[0]
    blocks = (group * width + jnp.bitwise_xor(member, jnp.arange(width))) * parts + depth
    spots = blocks[:, None] * rows + jnp.arange(rows)[None, :]
    firsts = doc_starts(doc_lengths, spots.reshape(-1)).reshape(width, rows).astype(jnp.int32)
    tables = (firsts[:, 0], firsts)

    def cut(value, k):
        size = value.shape[1] // width
        return lax.dynamic_slice_in_dim(value, jnp.bitwise_xor(member, k) * size, size, 1)

    ring = [(i, (i + 1) % parts) for i in range(parts)]
    pairs = [
        swap(jnp.concatenate([cut(packed_key_rows, k), cut(packed_value_rows, k)], axis=1), k)
        for k in range(width)
    ]
    opens = [(0, chunk // 2), (chunk // 2, chunk), (chunk, width)]
    queries = [swap(cut(packed_query_rows, k), k) for k in range(width)]

    def move(piece):
        return lax.ppermute(piece, "head", ring)

    held = [(low, jnp.stack(pairs[low:high])) for low, high in opens]
    pieces = [(0, low, piece) for low, piece in held]
    held = [(low, move(piece)) for low, piece in held]
    pieces += [(1, low, piece) for low, piece in held]
    held = [(0, jnp.concatenate([held[0][1], held[1][1]], axis=0)), held[2]]
    for step in range(2, parts):
        held = [(low, move(piece)) for low, piece in held]
        pieces += [(step, low, piece) for low, piece in held]

    attends = functools.partial(attend, place, tables, queries)
    everyone = list(range(width))
    soon = parts // 2
    first = [piece for piece in pieces if piece[0] < soon]
    state = attends(first, None, everyone, None, False, parts)
    late = [piece for piece in pieces if piece[0] >= soon]
    if docs > width:
        over = [(i, i + width) for i in range(docs - width)]
        far = [(step, low, lax.ppermute(piece, "doc", over)) for step, low, piece in pieces]
        state = attends(far, None, everyone, state, False, parts, back=1)
    near = [piece for piece in late if piece[1] < chunk]
    state = attends(near, 0, everyone, state, False, parts)
    results = {}
    for turn in reversed(range(HALVES)):
        slots = list(range(turn * chunk, (turn + 1) * chunk))
        rest = [piece for piece in late if piece[1] >= chunk]
        outs = attends(rest, 1, slots, state, True, parts)
        for slot, out in zip(slots, outs):
            results[slot] = swap(out, slot)
    return collect(place, [results[k] for k in range(width)])


def solution(mesh):
    in_specs = (P(("doc", "head"), None), P(("doc", "head"), None), P(("doc", "head"), None), P())
    out_specs = P(("doc", "head"), None)

    return jax.shard_map(
        on_device, mesh=mesh, in_specs=in_specs, out_specs=out_specs, check_vma=False
    )
```

```python
import functools
import math

import jax
import jax.numpy as jnp
from jax import lax
from jax.experimental import pallas as pl
from jax.experimental.pallas import tpu as pltpu
from jax.sharding import PartitionSpec as P


KEY_VALUE_HEADS = 8
HEAD_SIZE = 128
NEGATIVE = -1e30
HALVES = 2


def inside(value):
    return pltpu.with_memory_space_constraint(value, pltpu.VMEM)


def attend_kernel(
    pieces, half, back, slots, opening, closing, parts, place_ref, bounds_ref, firsts_ref, *refs
):
    width = KEY_VALUE_HEADS
    count = len(slots)
    steps = sorted({step for step, _ in pieces})
    q_refs, refs = refs[: count // 2], refs[count // 2 :]
    units, refs = refs[: len(pieces)], refs[len(pieces) :]
    if not opening:
        acc_in, stat_in = refs[:2]
        refs = refs[2:]
    if closing:
        out_refs, refs = refs[:count], refs[count:]
    acc_ref, stat_ref, score_ref, peak_ref, q_ref, kv_ref, list_ref = refs
    rows, columns = q_refs[0].shape[1:]
    heads = columns // HEAD_SIZE
    lanes = heads * rows
    shard = parts * rows
    depth = place_ref[0]
    member = place_ref[1]
    group = place_ref[2]
    origin = group - back
    scale = math.log2(math.e) / math.sqrt(HEAD_SIZE)
    if half is None:
        bottom, chunk = 0, width
    else:
        chunk = width // HALVES
        bottom = jnp.bitwise_xor(lax.div(member, chunk), half) * chunk

    visits = jnp.int32(0)
    for turn, slot in enumerate(slots):
        doc = jnp.bitwise_xor(member, slot) + back * width
        lowest = lax.div(bounds_ref[slot], shard) - origin * width
        start = jnp.maximum(lowest, bottom)
        stop = jnp.maximum(jnp.minimum(doc, bottom + chunk - 1) + 1, start)

        def note(key_doc, spot, turn=turn):
            list_ref[0, spot] = turn
            list_ref[1, spot] = key_doc
            return spot + 1

        visits = lax.fori_loop(start, stop, note, visits)

    for (step, first), unit in zip(pieces, units):
        at = steps.index(step) * rows
        kv_ref[first : first + unit.shape[0], at : at + rows, :] = unit[...]
    for i in range(count):
        for h in range(heads):
            q_ref[i, h * rows : (h + 1) * rows, :] = q_refs[i // 2][i % 2, :, h * HEAD_SIZE : (h + 1) * HEAD_SIZE]
    if opening:
        acc_ref[...] = jnp.zeros_like(acc_ref)
        stat_ref[:, 0:1, :] = jnp.full((count, 1, lanes), NEGATIVE, jnp.float32)
        stat_ref[:, 1:2, :] = jnp.zeros((count, 1, lanes), jnp.float32)
    else:
        acc_ref[...] = acc_in[slots[0] : slots[0] + count]
        stat_ref[...] = stat_in[slots[0] : slots[0] + count]

    def multiply(i):
        turn, key_doc = list_ref[0, i], list_ref[1, i]
        keys = kv_ref[jnp.bitwise_xor(member, key_doc), :, 0:HEAD_SIZE]
        return lax.dot_general(
            keys, q_ref[turn], (((1,), (1,)), ((), ())), preferred_element_type=jnp.float32
        )

    def settle(i, scores):
        turn, key_doc = list_ref[0, i], list_ref[1, i]
        slot = slots[0] + turn
        doc = jnp.bitwise_xor(member, slot)
        base = (origin * width + key_doc) * shard
        root = ((group * width + doc) * parts + depth) * rows
        at = root + lax.broadcasted_iota(jnp.int32, (1, rows), 1)
        firsts = firsts_ref[pl.ds(slot, 1), :]
        seen = []
        for step in steps:
            behind = depth - step
            behind = jnp.where(behind < 0, behind + parts, behind)
            spot = lax.broadcasted_iota(jnp.int32, (rows, rows), 0)
            corner = base + behind * rows
            here = (spot >= firsts - corner) & (spot <= at - corner)
            seen.append(jnp.concatenate([here] * heads, axis=1))
        scores = jnp.where(jnp.concatenate(seen, axis=0), scores, NEGATIVE)
        score_ref[...] = scores
        peak_ref[0:1, :] = jnp.max(scores, axis=0, keepdims=True)

    @pl.when(visits > 0)
    def _():
        settle(0, multiply(0))

        def visit(i, _):
            turn, key_doc = list_ref[0, i], list_ref[1, i]
            follow = jnp.minimum(i + 1, visits - 1)
            coming = multiply(follow)
            before = stat_ref[turn, 0:1, :]
            peak = jnp.maximum(before, peak_ref[0:1, :])
            weights = jnp.exp2((score_ref[...] - peak) * scale)
            total = jnp.sum(weights, axis=0, keepdims=True)
            values = kv_ref[jnp.bitwise_xor(member, key_doc), :, HEAD_SIZE:]
            gain = lax.dot_general(
                values,
                weights.astype(jnp.bfloat16),
                (((0,), (0,)), ((), ())),
                preferred_element_type=jnp.float32,
            )
            settle(follow, coming)
            shrink = jnp.exp2((before - peak) * scale)
            stat_ref[turn, 0:1, :] = peak
            stat_ref[turn, 1:2, :] = stat_ref[turn, 1:2, :] * shrink + total
            acc_ref[turn] = acc_ref[turn] * shrink + gain
            return 0

        lax.fori_loop(0, visits, visit, 0)

    if closing:
        for i in range(count):
            done = (acc_ref[i] / stat_ref[i, 1:2, :]).astype(out_refs[i].dtype)
            for h in range(heads):
                out_refs[i][:, h * HEAD_SIZE : (h + 1) * HEAD_SIZE] = done[:, h * rows : (h + 1) * rows].T


def attend(place, tables, queries, pieces, half, slots, state, closing, parts, back=0):
    width = KEY_VALUE_HEADS
    bounds, firsts = tables
    rows, columns = queries[0].shape[1:]
    lanes = columns // HEAD_SIZE * rows
    vmem = pl.BlockSpec(memory_space=pltpu.VMEM)
    smem = pl.BlockSpec(memory_space=pltpu.SMEM)
    opening = state is None
    held = () if opening else state
    count = len(slots)
    tokens = len({step for step, _, _ in pieces}) * rows
    kept = [
        pltpu.VMEM((count, HEAD_SIZE, lanes), jnp.float32),
        pltpu.VMEM((count, 8, lanes), jnp.float32),
    ]
    scratch = [
        pltpu.VMEM((tokens, lanes), jnp.float32),
        pltpu.VMEM((8, lanes), jnp.float32),
        pltpu.VMEM((count, lanes, HEAD_SIZE), queries[0].dtype),
        pltpu.VMEM((width, tokens, 2 * HEAD_SIZE), queries[0].dtype),
        pltpu.SMEM((2, width * width), jnp.int32),
    ]
    aliases = {}
    if closing:
        out_shape = [pltpu.VMEM((rows, columns), queries[0].dtype) for _ in slots]
        scratch = kept + scratch
    else:
        out_shape = kept
        first = 3 + count // 2 + len(pieces)
        aliases = {} if opening else {first: 0, first + 1: 1}
    work = count * 2 * tokens * lanes * HEAD_SIZE * 4
    return pl.pallas_call(
        functools.partial(
            attend_kernel,
            tuple((step, first) for step, first, _ in pieces),
            half,
            back,
            tuple(slots),
            opening,
            closing,
            parts,
        ),
        out_shape=out_shape,
        in_specs=[smem, smem] + [vmem] * (1 + count // 2 + len(pieces) + len(held)),
        out_specs=[vmem] * len(out_shape),
        input_output_aliases=aliases,
        cost_estimate=pl.CostEstimate(
            flops=work, bytes_accessed=4 * width * HEAD_SIZE * lanes, transcendentals=0
        ),
        scratch_shapes=scratch,
        compiler_params=pltpu.CompilerParams(vmem_limit_bytes=24 << 20),
    )(
        place,
        bounds,
        firsts,
        *[inside(queries[slot // 2]) for slot in slots[::2]],
        *[inside(unit) for _, _, unit in pieces],
        *[inside(part) for part in held],
    )


def collect_kernel(slots, place_ref, *refs):
    out_ref, sem = refs[-2:]
    copies = []
    for i, slot in enumerate(slots):
        columns = refs[i].shape[1]
        at = pl.multiple_of(jnp.bitwise_xor(place_ref[1], slot) * columns, columns)
        copies.append(pltpu.make_async_copy(refs[i], out_ref.at[:, pl.ds(at, columns)], sem.at[i]))
    for copy in copies:
        copy.start()
    for copy in copies:
        copy.wait()


def collect(place, blocks, slots, target):
    rows, columns = blocks[0].shape
    count = len(slots)
    smem = pl.BlockSpec(memory_space=pltpu.SMEM)
    vmem = pl.BlockSpec(memory_space=pltpu.VMEM)
    hbm = pl.BlockSpec(memory_space=pltpu.HBM)
    held = () if target is None else (target,)
    return pl.pallas_call(
        functools.partial(collect_kernel, tuple(slots)),
        out_shape=jax.ShapeDtypeStruct((rows, len(blocks) * columns), blocks[0].dtype),
        in_specs=[smem] + [vmem] * count + [hbm] * len(held),
        out_specs=hbm,
        input_output_aliases={1 + count: 0} if held else {},
        scratch_shapes=[pltpu.SemaphoreType.DMA((count,))],
        compiler_params=pltpu.CompilerParams(vmem_limit_bytes=4 << 20),
    )(place, *[inside(blocks[slot]) for slot in slots], *held)


def doc_starts(doc_lengths, positions):
    closing = jnp.cumsum(doc_lengths)
    passed = closing[None, :] <= positions[:, None]
    return jnp.sum(jnp.where(passed, doc_lengths[None, :], 0), axis=1)


def swap(block, k):
    if k == 0:
        return block
    length = lax.axis_size("doc")
    return lax.ppermute(block, "doc", [(i, i ^ k) for i in range(length)])


def on_device(packed_query_rows, packed_key_rows, packed_value_rows, doc_lengths):
    width = KEY_VALUE_HEADS
    chunk = width // HALVES
    docs, parts = lax.axis_size("doc"), lax.axis_size("head")
    index = lax.axis_index("doc")
    member, group = index % width, index // width
    depth = lax.axis_index("head")
    place = jnp.stack([depth, member, group]).astype(jnp.int32)
    rows = packed_query_rows.shape[0]
    blocks = (group * width + jnp.bitwise_xor(member, jnp.arange(width))) * parts + depth
    spots = blocks[:, None] * rows + jnp.arange(rows)[None, :]
    firsts = doc_starts(doc_lengths, spots.reshape(-1)).reshape(width, rows).astype(jnp.int32)
    tables = (firsts[:, 0], firsts)

    def cut(value, k):
        size = value.shape[1] // width
        return lax.dynamic_slice_in_dim(value, jnp.bitwise_xor(member, k) * size, size, 1)

    ring = [(i, (i + 1) % parts) for i in range(parts)]

    def pair(k):
        return jnp.concatenate([cut(packed_key_rows, k), cut(packed_value_rows, k)], axis=1)

    def spread(block):
        given = swap(jnp.stack([block(k) for k in range(1, width, 2)]), 1)
        both = []
        for k in range(0, width, 2):
            both.append(jnp.stack([block(k), given[k // 2]]))
        return [swap(value, 2 * t) for t, value in enumerate(both)]

    pairs = spread(pair)
    queries = spread(lambda k: cut(packed_query_rows, k))
    opens = [(0, chunk // 2), (chunk // 2, chunk), (chunk, width)]

    def move(piece):
        return lax.ppermute(piece, "head", ring)

    held = [(low, jnp.concatenate(pairs[low // 2 : high // 2])) for low, high in opens]
    pieces = [(0, low, piece) for low, piece in held]
    held = [(low, move(piece)) for low, piece in held]
    pieces += [(1, low, piece) for low, piece in held]
    held = [(0, jnp.concatenate([held[0][1], held[1][1]], axis=0)), held[2]]
    for step in range(2, parts):
        held = [(low, move(piece)) for low, piece in held]
        pieces += [(step, low, piece) for low, piece in held]

    attends = functools.partial(attend, place, tables, queries)
    everyone = list(range(width))
    soon = parts // 2
    first = [piece for piece in pieces if piece[0] < soon]
    state = attends(first, None, everyone, None, False, parts)
    late = [piece for piece in pieces if piece[0] >= soon]
    if docs > width:
        over = [(i, i + width) for i in range(docs - width)]
        far = [(step, low, lax.ppermute(piece, "doc", over)) for step, low, piece in pieces]
        state = attends(far, None, everyone, state, False, parts, back=1)
    near = [piece for piece in late if piece[1] < chunk]
    state = attends(near, 0, everyone, state, False, parts)
    results = {}
    for turn in reversed(range(HALVES)):
        slots = list(range(turn * chunk, (turn + 1) * chunk))
        rest = [piece for piece in late if piece[1] >= chunk]
        outs = attends(rest, 1, slots, state, True, parts)
        for slot, out in zip(slots, outs):
            results[slot] = swap(out, slot)
    blocks = [results[k] for k in range(width)]
    target = None
    for slots in [[0, *range(chunk, width)], list(range(1, chunk))]:
        target = collect(place, blocks, slots, target)
    return target


def solution(mesh):
    in_specs = (P(("doc", "head"), None), P(("doc", "head"), None), P(("doc", "head"), None), P())
    out_specs = P(("doc", "head"), None)

    return jax.shard_map(
        on_device, mesh=mesh, in_specs=in_specs, out_specs=out_specs, check_vma=False
    )
```

```python
import functools
import math

import jax
import jax.numpy as jnp
from jax import lax
from jax.experimental import pallas as pl
from jax.experimental.pallas import tpu as pltpu
from jax.sharding import PartitionSpec as P


KEY_VALUE_HEADS = 8
HEAD_SIZE = 128
NEGATIVE = -1e30
HALVES = 2


def inside(value):
    return pltpu.with_memory_space_constraint(value, pltpu.VMEM)


def attend_kernel(
    pieces, half, back, slots, opening, closing, parts, place_ref, bounds_ref, firsts_ref, *refs
):
    width = KEY_VALUE_HEADS
    count = len(slots)
    steps = sorted({step for step, _ in pieces})
    q_refs, refs = refs[: count // 2], refs[count // 2 :]
    units, refs = refs[: len(pieces)], refs[len(pieces) :]
    if not opening:
        acc_in, stat_in = refs[:2]
        refs = refs[2:]
    if closing:
        out_refs, refs = refs[:count], refs[count:]
    acc_ref, stat_ref, score_ref, peak_ref, q_ref, kv_ref, list_ref = refs
    rows, columns = q_refs[0].shape[1:]
    heads = columns // HEAD_SIZE
    lanes = heads * rows
    shard = parts * rows
    depth = place_ref[0]
    member = place_ref[1]
    group = place_ref[2]
    origin = group - back
    scale = math.log2(math.e) / math.sqrt(HEAD_SIZE)
    if half is None:
        bottom, chunk = 0, width
    else:
        chunk = width // HALVES
        bottom = jnp.bitwise_xor(lax.div(member, chunk), half) * chunk

    visits = jnp.int32(0)
    for turn, slot in enumerate(slots):
        doc = jnp.bitwise_xor(member, slot) + back * width
        lowest = lax.div(bounds_ref[slot], shard) - origin * width
        start = jnp.maximum(lowest, bottom)
        stop = jnp.maximum(jnp.minimum(doc, bottom + chunk - 1) + 1, start)

        def note(key_doc, spot, turn=turn):
            list_ref[0, spot] = turn
            list_ref[1, spot] = key_doc
            return spot + 1

        visits = lax.fori_loop(start, stop, note, visits)

    for (step, first), unit in zip(pieces, units):
        at = steps.index(step) * rows
        kv_ref[first : first + unit.shape[0], at : at + rows, :] = unit[...]
    for i in range(count):
        for h in range(heads):
            q_ref[i, h * rows : (h + 1) * rows, :] = q_refs[i // 2][i % 2, :, h * HEAD_SIZE : (h + 1) * HEAD_SIZE]
    if opening:
        acc_ref[...] = jnp.zeros_like(acc_ref)
        stat_ref[:, 0:1, :] = jnp.full((count, 1, lanes), NEGATIVE, jnp.float32)
        stat_ref[:, 1:2, :] = jnp.zeros((count, 1, lanes), jnp.float32)
    else:
        acc_ref[...] = acc_in[slots[0] : slots[0] + count]
        stat_ref[...] = stat_in[slots[0] : slots[0] + count]

    def multiply(i):
        turn, key_doc = list_ref[0, i], list_ref[1, i]
        keys = kv_ref[jnp.bitwise_xor(member, key_doc), :, 0:HEAD_SIZE]
        return lax.dot_general(
            keys, q_ref[turn], (((1,), (1,)), ((), ())), preferred_element_type=jnp.float32
        )

    def settle(i, scores):
        turn, key_doc = list_ref[0, i], list_ref[1, i]
        slot = slots[0] + turn
        doc = jnp.bitwise_xor(member, slot)
        base = (origin * width + key_doc) * shard
        root = ((group * width + doc) * parts + depth) * rows
        at = root + lax.broadcasted_iota(jnp.int32, (1, rows), 1)
        firsts = firsts_ref[pl.ds(slot, 1), :]
        seen = []
        for step in steps:
            behind = depth - step
            behind = jnp.where(behind < 0, behind + parts, behind)
            spot = lax.broadcasted_iota(jnp.int32, (rows, rows), 0)
            corner = base + behind * rows
            here = (spot >= firsts - corner) & (spot <= at - corner)
            seen.append(jnp.concatenate([here] * heads, axis=1))
        scores = jnp.where(jnp.concatenate(seen, axis=0), scores, NEGATIVE)
        score_ref[...] = scores
        peak_ref[0:1, :] = jnp.max(scores, axis=0, keepdims=True)

    @pl.when(visits > 0)
    def _():
        settle(0, multiply(0))

        def visit(i, _):
            turn, key_doc = list_ref[0, i], list_ref[1, i]
            follow = jnp.minimum(i + 1, visits - 1)
            coming = multiply(follow)
            before = stat_ref[turn, 0:1, :]
            peak = jnp.maximum(before, peak_ref[0:1, :])
            weights = jnp.exp2((score_ref[...] - peak) * scale)
            total = jnp.sum(weights, axis=0, keepdims=True)
            values = kv_ref[jnp.bitwise_xor(member, key_doc), :, HEAD_SIZE:]
            gain = lax.dot_general(
                values,
                weights.astype(jnp.bfloat16),
                (((0,), (0,)), ((), ())),
                preferred_element_type=jnp.float32,
            )
            settle(follow, coming)
            shrink = jnp.exp2((before - peak) * scale)
            stat_ref[turn, 0:1, :] = peak
            stat_ref[turn, 1:2, :] = stat_ref[turn, 1:2, :] * shrink + total
            acc_ref[turn] = acc_ref[turn] * shrink + gain
            return 0

        lax.fori_loop(0, visits, visit, 0)

    if closing:
        for i in range(count):
            done = (acc_ref[i] / stat_ref[i, 1:2, :]).astype(out_refs[i].dtype)
            for h in range(heads):
                out_refs[i][:, h * HEAD_SIZE : (h + 1) * HEAD_SIZE] = done[:, h * rows : (h + 1) * rows].T


def attend(place, tables, queries, pieces, half, slots, state, closing, parts, back=0):
    width = KEY_VALUE_HEADS
    bounds, firsts = tables
    rows, columns = queries[0].shape[1:]
    lanes = columns // HEAD_SIZE * rows
    vmem = pl.BlockSpec(memory_space=pltpu.VMEM)
    smem = pl.BlockSpec(memory_space=pltpu.SMEM)
    opening = state is None
    held = () if opening else state
    count = len(slots)
    tokens = len({step for step, _, _ in pieces}) * rows
    kept = [
        pltpu.VMEM((count, HEAD_SIZE, lanes), jnp.float32),
        pltpu.VMEM((count, 8, lanes), jnp.float32),
    ]
    scratch = [
        pltpu.VMEM((tokens, lanes), jnp.float32),
        pltpu.VMEM((8, lanes), jnp.float32),
        pltpu.VMEM((count, lanes, HEAD_SIZE), queries[0].dtype),
        pltpu.VMEM((width, tokens, 2 * HEAD_SIZE), queries[0].dtype),
        pltpu.SMEM((2, width * width), jnp.int32),
    ]
    aliases = {}
    if closing:
        out_shape = [pltpu.VMEM((rows, columns), queries[0].dtype) for _ in slots]
        scratch = kept + scratch
    else:
        out_shape = kept
        first = 3 + count // 2 + len(pieces)
        aliases = {} if opening else {first: 0, first + 1: 1}
    work = count * 2 * tokens * lanes * HEAD_SIZE * 4
    return pl.pallas_call(
        functools.partial(
            attend_kernel,
            tuple((step, first) for step, first, _ in pieces),
            half,
            back,
            tuple(slots),
            opening,
            closing,
            parts,
        ),
        out_shape=out_shape,
        in_specs=[smem, smem] + [vmem] * (1 + count // 2 + len(pieces) + len(held)),
        out_specs=[vmem] * len(out_shape),
        input_output_aliases=aliases,
        cost_estimate=pl.CostEstimate(
            flops=work, bytes_accessed=4 * width * HEAD_SIZE * lanes, transcendentals=0
        ),
        scratch_shapes=scratch,
        compiler_params=pltpu.CompilerParams(vmem_limit_bytes=24 << 20),
    )(
        place,
        bounds,
        firsts,
        *[inside(queries[slot // 2]) for slot in slots[::2]],
        *[inside(unit) for _, _, unit in pieces],
        *[inside(part) for part in held],
    )


def collect_kernel(place_ref, *refs):
    sem = refs[-1]
    out_ref = refs[-2]
    copies = []
    for k, ref in enumerate(refs[:-2]):
        columns = ref.shape[1]
        at = pl.multiple_of(jnp.bitwise_xor(place_ref[1], k) * columns, columns)
        copies.append(pltpu.make_async_copy(ref, out_ref.at[:, pl.ds(at, columns)], sem.at[k]))
    for copy in copies:
        copy.start()
    for copy in copies:
        copy.wait()


def collect(place, blocks):
    rows, columns = blocks[0].shape
    count = len(blocks)
    return pl.pallas_call(
        collect_kernel,
        out_shape=jax.ShapeDtypeStruct((rows, count * columns), blocks[0].dtype),
        in_specs=[pl.BlockSpec(memory_space=pltpu.SMEM)]
        + [pl.BlockSpec(memory_space=pltpu.VMEM)] * count,
        out_specs=pl.BlockSpec(memory_space=pltpu.HBM),
        scratch_shapes=[pltpu.SemaphoreType.DMA((count,))],
        compiler_params=pltpu.CompilerParams(vmem_limit_bytes=4 << 20),
    )(place, *[inside(block) for block in blocks])


def doc_starts(doc_lengths, positions):
    closing = jnp.cumsum(doc_lengths)
    passed = closing[None, :] <= positions[:, None]
    return jnp.sum(jnp.where(passed, doc_lengths[None, :], 0), axis=1)


def swap(block, k):
    if k == 0:
        return block
    length = lax.axis_size("doc")
    return lax.ppermute(block, "doc", [(i, i ^ k) for i in range(length)])


def on_device(packed_query_rows, packed_key_rows, packed_value_rows, doc_lengths):
    width = KEY_VALUE_HEADS
    chunk = width // HALVES
    docs, parts = lax.axis_size("doc"), lax.axis_size("head")
    index = lax.axis_index("doc")
    member, group = index % width, index // width
    depth = lax.axis_index("head")
    place = jnp.stack([depth, member, group]).astype(jnp.int32)
    rows = packed_query_rows.shape[0]
    blocks = (group * width + jnp.bitwise_xor(member, jnp.arange(width))) * parts + depth
    spots = blocks[:, None] * rows + jnp.arange(rows)[None, :]
    firsts = doc_starts(doc_lengths, spots.reshape(-1)).reshape(width, rows).astype(jnp.int32)
    tables = (firsts[:, 0], firsts)

    def cut(value, k):
        size = value.shape[1] // width
        return lax.dynamic_slice_in_dim(value, jnp.bitwise_xor(member, k) * size, size, 1)

    ring = [(i, (i + 1) % parts) for i in range(parts)]

    def pair(k):
        return jnp.concatenate([cut(packed_key_rows, k), cut(packed_value_rows, k)], axis=1)

    def spread(block):
        given = swap(jnp.stack([block(k) for k in range(1, width, 2)]), 1)
        both = []
        for k in range(0, width, 2):
            both.append(jnp.stack([block(k), given[k // 2]]))
        return [swap(value, 2 * t) for t, value in enumerate(both)]

    pairs = spread(pair)
    queries = spread(lambda k: cut(packed_query_rows, k))
    opens = [(0, chunk // 2), (chunk // 2, chunk), (chunk, width)]

    def move(piece):
        return lax.ppermute(piece, "head", ring)

    held = [(low, jnp.concatenate(pairs[low // 2 : high // 2])) for low, high in opens]
    pieces = [(0, low, piece) for low, piece in held]
    held = [(low, move(piece)) for low, piece in held]
    pieces += [(1, low, piece) for low, piece in held]
    held = [(0, jnp.concatenate([held[0][1], held[1][1]], axis=0)), held[2]]
    for step in range(2, parts):
        held = [(low, move(piece)) for low, piece in held]
        pieces += [(step, low, piece) for low, piece in held]

    attends = functools.partial(attend, place, tables, queries)
    everyone = list(range(width))
    soon = parts // 2
    first = [piece for piece in pieces if piece[0] < soon]
    state = attends(first, None, everyone, None, False, parts)
    late = [piece for piece in pieces if piece[0] >= soon]
    if docs > width:
        over = [(i, i + width) for i in range(docs - width)]
        far = [(step, low, lax.ppermute(piece, "doc", over)) for step, low, piece in pieces]
        state = attends(far, None, everyone, state, False, parts, back=1)
    near = [piece for piece in late if piece[1] < chunk]
    state = attends(near, 0, everyone, state, False, parts)
    results = {}
    for turn in reversed(range(HALVES)):
        slots = list(range(turn * chunk, (turn + 1) * chunk))
        rest = [piece for piece in late if piece[1] >= chunk]
        outs = attends(rest, 1, slots, state, True, parts)
        for slot, out in zip(slots, outs):
            results[slot] = swap(out, slot)
    return collect(place, [results[k] for k in range(width)])


def solution(mesh):
    in_specs = (P(("doc", "head"), None), P(("doc", "head"), None), P(("doc", "head"), None), P())
    out_specs = P(("doc", "head"), None)

    return jax.shard_map(
        on_device, mesh=mesh, in_specs=in_specs, out_specs=out_specs, check_vma=False
    )
```

```python
import functools
import math

import jax
import jax.numpy as jnp
from jax import lax
from jax.experimental import pallas as pl
from jax.experimental.pallas import tpu as pltpu
from jax.sharding import PartitionSpec as P


KEY_VALUE_HEADS = 8
HEAD_SIZE = 128
NEGATIVE = -1e30
HALVES = 2


def inside(value):
    return pltpu.with_memory_space_constraint(value, pltpu.VMEM)


def attend_kernel(
    pieces, half, back, slots, opening, closing, parts, place_ref, bounds_ref, firsts_ref, *refs
):
    width = KEY_VALUE_HEADS
    count = len(slots)
    steps = sorted({step for step, _ in pieces})
    q_refs, refs = refs[: count // 2], refs[count // 2 :]
    units, refs = refs[: len(pieces)], refs[len(pieces) :]
    if not opening:
        acc_in, stat_in = refs[:2]
        refs = refs[2:]
    if closing:
        out_refs, refs = refs[:count], refs[count:]
    acc_ref, stat_ref, score_ref, peak_ref, q_ref, kv_ref, list_ref = refs
    rows, columns = q_refs[0].shape[1:]
    heads = columns // HEAD_SIZE
    lanes = heads * rows
    shard = parts * rows
    depth = place_ref[0]
    member = place_ref[1]
    group = place_ref[2]
    origin = group - back
    scale = math.log2(math.e) / math.sqrt(HEAD_SIZE)
    if half is None:
        bottom, chunk = 0, width
    else:
        chunk = width // HALVES
        bottom = jnp.bitwise_xor(lax.div(member, chunk), half) * chunk

    visits = jnp.int32(0)
    for turn, slot in enumerate(slots):
        doc = jnp.bitwise_xor(member, slot) + back * width
        lowest = lax.div(bounds_ref[slot], shard) - origin * width
        start = jnp.maximum(lowest, bottom)
        stop = jnp.maximum(jnp.minimum(doc, bottom + chunk - 1) + 1, start)

        def note(key_doc, spot, turn=turn):
            list_ref[0, spot] = turn
            list_ref[1, spot] = key_doc
            return spot + 1

        visits = lax.fori_loop(start, stop, note, visits)

    for (step, first), unit in zip(pieces, units):
        at = steps.index(step) * rows
        kv_ref[first : first + unit.shape[0], at : at + rows, :] = unit[...]
    for i in range(count):
        for h in range(heads):
            q_ref[i, h * rows : (h + 1) * rows, :] = q_refs[i // 2][i % 2, :, h * HEAD_SIZE : (h + 1) * HEAD_SIZE]
    if opening:
        acc_ref[...] = jnp.zeros_like(acc_ref)
        stat_ref[:, 0:1, :] = jnp.full((count, 1, lanes), NEGATIVE, jnp.float32)
        stat_ref[:, 1:2, :] = jnp.zeros((count, 1, lanes), jnp.float32)
    else:
        acc_ref[...] = acc_in[slots[0] : slots[0] + count]
        stat_ref[...] = stat_in[slots[0] : slots[0] + count]

    def multiply(i):
        turn, key_doc = list_ref[0, i], list_ref[1, i]
        keys = kv_ref[jnp.bitwise_xor(member, key_doc), :, 0:HEAD_SIZE]
        return lax.dot_general(
            keys, q_ref[turn], (((1,), (1,)), ((), ())), preferred_element_type=jnp.float32
        )

    def settle(i, scores):
        turn, key_doc = list_ref[0, i], list_ref[1, i]
        slot = slots[0] + turn
        doc = jnp.bitwise_xor(member, slot)
        base = (origin * width + key_doc) * shard
        root = ((group * width + doc) * parts + depth) * rows
        at = root + lax.broadcasted_iota(jnp.int32, (1, rows), 1)
        firsts = firsts_ref[pl.ds(slot, 1), :]
        seen = []
        for step in steps:
            behind = place_ref[3 + step]
            spot = lax.broadcasted_iota(jnp.int32, (rows, rows), 0)
            corner = base + behind * rows
            here = (spot >= firsts - corner) & (spot <= at - corner)
            seen.append(jnp.concatenate([here] * heads, axis=1))
        scores = jnp.where(jnp.concatenate(seen, axis=0), scores, NEGATIVE)
        score_ref[...] = scores
        peak_ref[0:1, :] = jnp.max(scores, axis=0, keepdims=True)

    @pl.when(visits > 0)
    def _():
        settle(0, multiply(0))

        def visit(i, _):
            turn, key_doc = list_ref[0, i], list_ref[1, i]
            follow = jnp.minimum(i + 1, visits - 1)
            coming = multiply(follow)
            before = stat_ref[turn, 0:1, :]
            peak = jnp.maximum(before, peak_ref[0:1, :])
            weights = jnp.exp2((score_ref[...] - peak) * scale)
            total = jnp.sum(weights, axis=0, keepdims=True)
            values = kv_ref[jnp.bitwise_xor(member, key_doc), :, HEAD_SIZE:]
            gain = lax.dot_general(
                values,
                weights.astype(jnp.bfloat16),
                (((0,), (0,)), ((), ())),
                preferred_element_type=jnp.float32,
            )
            settle(follow, coming)
            shrink = jnp.exp2((before - peak) * scale)
            stat_ref[turn, 0:1, :] = peak
            stat_ref[turn, 1:2, :] = stat_ref[turn, 1:2, :] * shrink + total
            acc_ref[turn] = acc_ref[turn] * shrink + gain
            return 0

        lax.fori_loop(0, visits, visit, 0)

    if closing:
        for i in range(count):
            done = (acc_ref[i] / stat_ref[i, 1:2, :]).astype(out_refs[i].dtype)
            for h in range(heads):
                out_refs[i][:, h * HEAD_SIZE : (h + 1) * HEAD_SIZE] = done[:, h * rows : (h + 1) * rows].T


def attend(place, tables, queries, pieces, half, slots, state, closing, parts, back=0):
    width = KEY_VALUE_HEADS
    bounds, firsts = tables
    rows, columns = queries[0].shape[1:]
    lanes = columns // HEAD_SIZE * rows
    vmem = pl.BlockSpec(memory_space=pltpu.VMEM)
    smem = pl.BlockSpec(memory_space=pltpu.SMEM)
    opening = state is None
    held = () if opening else state
    count = len(slots)
    tokens = len({step for step, _, _ in pieces}) * rows
    kept = [
        pltpu.VMEM((count, HEAD_SIZE, lanes), jnp.float32),
        pltpu.VMEM((count, 8, lanes), jnp.float32),
    ]
    scratch = [
        pltpu.VMEM((tokens, lanes), jnp.float32),
        pltpu.VMEM((8, lanes), jnp.float32),
        pltpu.VMEM((count, lanes, HEAD_SIZE), queries[0].dtype),
        pltpu.VMEM((width, tokens, 2 * HEAD_SIZE), queries[0].dtype),
        pltpu.SMEM((2, width * width), jnp.int32),
    ]
    aliases = {}
    if closing:
        out_shape = [pltpu.VMEM((rows, columns), queries[0].dtype) for _ in slots]
        scratch = kept + scratch
    else:
        out_shape = kept
        first = 3 + count // 2 + len(pieces)
        aliases = {} if opening else {first: 0, first + 1: 1}
    work = count * 2 * tokens * lanes * HEAD_SIZE * 4
    return pl.pallas_call(
        functools.partial(
            attend_kernel,
            tuple((step, first) for step, first, _ in pieces),
            half,
            back,
            tuple(slots),
            opening,
            closing,
            parts,
        ),
        out_shape=out_shape,
        in_specs=[smem, smem] + [vmem] * (1 + count // 2 + len(pieces) + len(held)),
        out_specs=[vmem] * len(out_shape),
        input_output_aliases=aliases,
        cost_estimate=pl.CostEstimate(
            flops=work, bytes_accessed=4 * width * HEAD_SIZE * lanes, transcendentals=0
        ),
        scratch_shapes=scratch,
        compiler_params=pltpu.CompilerParams(vmem_limit_bytes=24 << 20),
    )(
        place,
        bounds,
        firsts,
        *[inside(queries[slot // 2]) for slot in slots[::2]],
        *[inside(unit) for _, _, unit in pieces],
        *[inside(part) for part in held],
    )


def collect_kernel(place_ref, *refs):
    sem = refs[-1]
    out_ref = refs[-2]
    copies = []
    for k, ref in enumerate(refs[:-2]):
        columns = ref.shape[1]
        at = pl.multiple_of(jnp.bitwise_xor(place_ref[1], k) * columns, columns)
        copies.append(pltpu.make_async_copy(ref, out_ref.at[:, pl.ds(at, columns)], sem.at[k]))
    for copy in copies:
        copy.start()
    for copy in copies:
        copy.wait()


def collect(place, blocks):
    rows, columns = blocks[0].shape
    count = len(blocks)
    return pl.pallas_call(
        collect_kernel,
        out_shape=jax.ShapeDtypeStruct((rows, count * columns), blocks[0].dtype),
        in_specs=[pl.BlockSpec(memory_space=pltpu.SMEM)]
        + [pl.BlockSpec(memory_space=pltpu.VMEM)] * count,
        out_specs=pl.BlockSpec(memory_space=pltpu.HBM),
        scratch_shapes=[pltpu.SemaphoreType.DMA((count,))],
        compiler_params=pltpu.CompilerParams(vmem_limit_bytes=4 << 20),
    )(place, *[inside(block) for block in blocks])


def doc_starts(doc_lengths, positions):
    closing = jnp.cumsum(doc_lengths)
    passed = closing[None, :] <= positions[:, None]
    return jnp.sum(jnp.where(passed, doc_lengths[None, :], 0), axis=1)


def swap(block, k):
    if k == 0:
        return block
    length = lax.axis_size("doc")
    return lax.ppermute(block, "doc", [(i, i ^ k) for i in range(length)])


def on_device(packed_query_rows, packed_key_rows, packed_value_rows, doc_lengths):
    width = KEY_VALUE_HEADS
    chunk = width // HALVES
    docs, parts = lax.axis_size("doc"), lax.axis_size("head")
    index = lax.axis_index("doc")
    member, group = index % width, index // width
    depth = lax.axis_index("head")
    fold = [0, *range(1, parts, 2), *reversed(range(2, parts, 2))]
    ahead = [fold.index(z) for z in range(parts)]
    origins = [[fold[(ahead[z] - step) % parts] for step in range(parts)] for z in range(parts)]
    sources = jnp.asarray(origins, jnp.int32)[depth]
    place = jnp.concatenate([jnp.stack([depth, member, group]).astype(jnp.int32), sources])
    rows = packed_query_rows.shape[0]
    blocks = (group * width + jnp.bitwise_xor(member, jnp.arange(width))) * parts + depth
    spots = blocks[:, None] * rows + jnp.arange(rows)[None, :]
    firsts = doc_starts(doc_lengths, spots.reshape(-1)).reshape(width, rows).astype(jnp.int32)
    tables = (firsts[:, 0], firsts)

    def cut(value, k):
        size = value.shape[1] // width
        return lax.dynamic_slice_in_dim(value, jnp.bitwise_xor(member, k) * size, size, 1)

    ring = [(fold[i], fold[(i + 1) % parts]) for i in range(parts)]

    def pair(k):
        return jnp.concatenate([cut(packed_key_rows, k), cut(packed_value_rows, k)], axis=1)

    def spread(block):
        given = swap(jnp.stack([block(k) for k in range(1, width, 2)]), 1)
        both = []
        for k in range(0, width, 2):
            both.append(jnp.stack([block(k), given[k // 2]]))
        return [swap(value, 2 * t) for t, value in enumerate(both)]

    pairs = spread(pair)
    queries = spread(lambda k: cut(packed_query_rows, k))
    opens = [(0, chunk // 2), (chunk // 2, chunk), (chunk, width)]

    def move(piece):
        return lax.ppermute(piece, "head", ring)

    held = [(low, jnp.concatenate(pairs[low // 2 : high // 2])) for low, high in opens]
    pieces = [(0, low, piece) for low, piece in held]
    held = [(low, move(piece)) for low, piece in held]
    pieces += [(1, low, piece) for low, piece in held]
    held = [(0, jnp.concatenate([held[0][1], held[1][1]], axis=0)), held[2]]
    for step in range(2, parts):
        held = [(low, move(piece)) for low, piece in held]
        pieces += [(step, low, piece) for low, piece in held]

    attends = functools.partial(attend, place, tables, queries)
    everyone = list(range(width))
    soon = parts // 2
    first = [piece for piece in pieces if piece[0] < soon]
    state = attends(first, None, everyone, None, False, parts)
    late = [piece for piece in pieces if piece[0] >= soon]
    if docs > width:
        over = [(i, i + width) for i in range(docs - width)]
        far = [(step, low, lax.ppermute(piece, "doc", over)) for step, low, piece in pieces]
        state = attends(far, None, everyone, state, False, parts, back=1)
    near = [piece for piece in late if piece[1] < chunk]
    state = attends(near, 0, everyone, state, False, parts)
    results = {}
    for slots in (everyone[-2:], everyone[:-2]):
        rest = [piece for piece in late if piece[1] >= chunk]
        outs = attends(rest, 1, slots, state, True, parts)
        for slot, out in zip(slots, outs):
            results[slot] = swap(out, slot)
    return collect(place, [results[k] for k in range(width)])


def solution(mesh):
    in_specs = (P(("doc", "head"), None), P(("doc", "head"), None), P(("doc", "head"), None), P())
    out_specs = P(("doc", "head"), None)

    return jax.shard_map(
        on_device, mesh=mesh, in_specs=in_specs, out_specs=out_specs, check_vma=False
    )
```

```python
import functools
import math

import jax
import jax.numpy as jnp
from jax import lax
from jax.experimental import pallas as pl
from jax.experimental.pallas import tpu as pltpu
from jax.sharding import PartitionSpec as P


KEY_VALUE_HEADS = 8
HEAD_SIZE = 128
NEGATIVE = -1e30
HALVES = 2


def inside(value):
    return pltpu.with_memory_space_constraint(value, pltpu.VMEM)


def attend_kernel(
    pieces, half, back, slots, spans, closing, parts, place_ref, bounds_ref, firsts_ref, *refs
):
    width = KEY_VALUE_HEADS
    count = len(slots)
    steps = sorted({step for step, _ in pieces})
    q_refs, refs = refs[: count // 2], refs[count // 2 :]
    units, refs = refs[: len(pieces)], refs[len(pieces) :]
    kept, refs = refs[: 2 * len(spans)], refs[2 * len(spans) :]
    if closing:
        out_refs, refs = refs[:count], refs[count:]
    acc_ref, stat_ref, score_ref, peak_ref, q_ref, kv_ref, list_ref = refs
    rows, columns = q_refs[0].shape[1:]
    heads = columns // HEAD_SIZE
    lanes = heads * rows
    shard = parts * rows
    depth = place_ref[0]
    member = place_ref[1]
    group = place_ref[2]
    origin = group - back
    scale = math.log2(math.e) / math.sqrt(HEAD_SIZE)
    if half is None:
        bottom, chunk = 0, width
    else:
        chunk = width // HALVES
        bottom = jnp.bitwise_xor(lax.div(member, chunk), half) * chunk

    visits = jnp.int32(0)
    for turn, slot in enumerate(slots):
        doc = jnp.bitwise_xor(member, slot) + back * width
        lowest = lax.div(bounds_ref[slot], shard) - origin * width
        start = jnp.maximum(lowest, bottom)
        stop = jnp.maximum(jnp.minimum(doc, bottom + chunk - 1) + 1, start)

        def note(key_doc, spot, turn=turn):
            list_ref[0, spot] = turn
            list_ref[1, spot] = key_doc
            return spot + 1

        visits = lax.fori_loop(start, stop, note, visits)

    for (step, first), unit in zip(pieces, units):
        at = steps.index(step) * rows
        kv_ref[first : first + unit.shape[0], at : at + rows, :] = unit[...]
    for i in range(count):
        for h in range(heads):
            q_ref[i, h * rows : (h + 1) * rows, :] = q_refs[i // 2][i % 2, :, h * HEAD_SIZE : (h + 1) * HEAD_SIZE]
    if not spans:
        acc_ref[...] = jnp.zeros_like(acc_ref)
        stat_ref[:, 0:1, :] = jnp.full((count, 1, lanes), NEGATIVE, jnp.float32)
        stat_ref[:, 1:2, :] = jnp.zeros((count, 1, lanes), jnp.float32)
    for i, (first, size) in enumerate(spans):
        low, high = max(first, slots[0]), min(first + size, slots[0] + count)
        if low < high:
            to, source = slice(low - slots[0], high - slots[0]), slice(low - first, high - first)
            acc_ref[to] = kept[2 * i][source]
            stat_ref[to] = kept[2 * i + 1][source]

    def multiply(i):
        turn, key_doc = list_ref[0, i], list_ref[1, i]
        keys = kv_ref[jnp.bitwise_xor(member, key_doc), :, 0:HEAD_SIZE]
        return lax.dot_general(
            keys, q_ref[turn], (((1,), (1,)), ((), ())), preferred_element_type=jnp.float32
        )

    def settle(i, scores):
        turn, key_doc = list_ref[0, i], list_ref[1, i]
        slot = slots[0] + turn
        doc = jnp.bitwise_xor(member, slot)
        base = (origin * width + key_doc) * shard
        root = ((group * width + doc) * parts + depth) * rows
        at = root + lax.broadcasted_iota(jnp.int32, (1, rows), 1)
        firsts = firsts_ref[pl.ds(slot, 1), :]
        seen = []
        for step in steps:
            behind = place_ref[3 + step]
            spot = lax.broadcasted_iota(jnp.int32, (rows, rows), 0)
            corner = base + behind * rows
            here = (spot >= firsts - corner) & (spot <= at - corner)
            seen.append(jnp.concatenate([here] * heads, axis=1))
        scores = jnp.where(jnp.concatenate(seen, axis=0), scores, NEGATIVE)
        score_ref[...] = scores
        peak_ref[0:1, :] = jnp.max(scores, axis=0, keepdims=True)

    @pl.when(visits > 0)
    def _():
        settle(0, multiply(0))

        def visit(i, _):
            turn, key_doc = list_ref[0, i], list_ref[1, i]
            follow = jnp.minimum(i + 1, visits - 1)
            coming = multiply(follow)
            before = stat_ref[turn, 0:1, :]
            peak = jnp.maximum(before, peak_ref[0:1, :])
            weights = jnp.exp2((score_ref[...] - peak) * scale)
            total = jnp.sum(weights, axis=0, keepdims=True)
            values = kv_ref[jnp.bitwise_xor(member, key_doc), :, HEAD_SIZE:]
            gain = lax.dot_general(
                values,
                weights.astype(jnp.bfloat16),
                (((0,), (0,)), ((), ())),
                preferred_element_type=jnp.float32,
            )
            settle(follow, coming)
            shrink = jnp.exp2((before - peak) * scale)
            stat_ref[turn, 0:1, :] = peak
            stat_ref[turn, 1:2, :] = stat_ref[turn, 1:2, :] * shrink + total
            acc_ref[turn] = acc_ref[turn] * shrink + gain
            return 0

        lax.fori_loop(0, visits, visit, 0)

    if closing:
        for i in range(count):
            done = (acc_ref[i] / stat_ref[i, 1:2, :]).astype(out_refs[i].dtype)
            for h in range(heads):
                out_refs[i][:, h * HEAD_SIZE : (h + 1) * HEAD_SIZE] = done[:, h * rows : (h + 1) * rows].T


def attend(place, tables, queries, pieces, half, slots, state, closing, parts, back=0):
    width = KEY_VALUE_HEADS
    bounds, firsts = tables
    rows, columns = queries[0].shape[1:]
    lanes = columns // HEAD_SIZE * rows
    vmem = pl.BlockSpec(memory_space=pltpu.VMEM)
    smem = pl.BlockSpec(memory_space=pltpu.SMEM)
    spans = tuple((first, acc.shape[0]) for first, acc, _ in state)
    held = [part for _, acc, stat in state for part in (acc, stat)]
    count = len(slots)
    tokens = len({step for step, _, _ in pieces}) * rows
    kept = [
        pltpu.VMEM((count, HEAD_SIZE, lanes), jnp.float32),
        pltpu.VMEM((count, 8, lanes), jnp.float32),
    ]
    scratch = [
        pltpu.VMEM((tokens, lanes), jnp.float32),
        pltpu.VMEM((8, lanes), jnp.float32),
        pltpu.VMEM((count, lanes, HEAD_SIZE), queries[0].dtype),
        pltpu.VMEM((width, tokens, 2 * HEAD_SIZE), queries[0].dtype),
        pltpu.SMEM((2, width * width), jnp.int32),
    ]
    aliases = {}
    if closing:
        out_shape = [pltpu.VMEM((rows, columns), queries[0].dtype) for _ in slots]
        scratch = kept + scratch
    else:
        out_shape = kept
        first = 3 + count // 2 + len(pieces)
        aliases = {first: 0, first + 1: 1} if spans == ((slots[0], count),) else {}
    work = count * 2 * tokens * lanes * HEAD_SIZE * 4
    return pl.pallas_call(
        functools.partial(
            attend_kernel,
            tuple((step, first) for step, first, _ in pieces),
            half,
            back,
            tuple(slots),
            spans,
            closing,
            parts,
        ),
        out_shape=out_shape,
        in_specs=[smem, smem] + [vmem] * (1 + count // 2 + len(pieces) + len(held)),
        out_specs=[vmem] * len(out_shape),
        input_output_aliases=aliases,
        cost_estimate=pl.CostEstimate(
            flops=work, bytes_accessed=4 * width * HEAD_SIZE * lanes, transcendentals=0
        ),
        scratch_shapes=scratch,
        compiler_params=pltpu.CompilerParams(vmem_limit_bytes=24 << 20),
    )(
        place,
        bounds,
        firsts,
        *[inside(queries[slot // 2]) for slot in slots[::2]],
        *[inside(unit) for _, _, unit in pieces],
        *[inside(part) for part in held],
    )


def collect_kernel(place_ref, *refs):
    sem = refs[-1]
    out_ref = refs[-2]
    copies = []
    for k, ref in enumerate(refs[:-2]):
        columns = ref.shape[1]
        at = pl.multiple_of(jnp.bitwise_xor(place_ref[1], k) * columns, columns)
        copies.append(pltpu.make_async_copy(ref, out_ref.at[:, pl.ds(at, columns)], sem.at[k]))
    for copy in copies:
        copy.start()
    for copy in copies:
        copy.wait()


def collect(place, blocks):
    rows, columns = blocks[0].shape
    count = len(blocks)
    return pl.pallas_call(
        collect_kernel,
        out_shape=jax.ShapeDtypeStruct((rows, count * columns), blocks[0].dtype),
        in_specs=[pl.BlockSpec(memory_space=pltpu.SMEM)]
        + [pl.BlockSpec(memory_space=pltpu.VMEM)] * count,
        out_specs=pl.BlockSpec(memory_space=pltpu.HBM),
        scratch_shapes=[pltpu.SemaphoreType.DMA((count,))],
        compiler_params=pltpu.CompilerParams(vmem_limit_bytes=4 << 20),
    )(place, *[inside(block) for block in blocks])


def doc_starts(doc_lengths, positions):
    closing = jnp.cumsum(doc_lengths)
    passed = closing[None, :] <= positions[:, None]
    return jnp.sum(jnp.where(passed, doc_lengths[None, :], 0), axis=1)


def swap(block, k):
    if k == 0:
        return block
    length = lax.axis_size("doc")
    return lax.ppermute(block, "doc", [(i, i ^ k) for i in range(length)])


def on_device(packed_query_rows, packed_key_rows, packed_value_rows, doc_lengths):
    width = KEY_VALUE_HEADS
    chunk = width // HALVES
    docs, parts = lax.axis_size("doc"), lax.axis_size("head")
    index = lax.axis_index("doc")
    member, group = index % width, index // width
    depth = lax.axis_index("head")
    fold = [0, *range(1, parts, 2), *reversed(range(2, parts, 2))]
    ahead = [fold.index(z) for z in range(parts)]
    origins = [[fold[(ahead[z] - step) % parts] for step in range(parts)] for z in range(parts)]
    sources = jnp.asarray(origins, jnp.int32)[depth]
    place = jnp.concatenate([jnp.stack([depth, member, group]).astype(jnp.int32), sources])
    rows = packed_query_rows.shape[0]
    blocks = (group * width + jnp.bitwise_xor(member, jnp.arange(width))) * parts + depth
    spots = blocks[:, None] * rows + jnp.arange(rows)[None, :]
    firsts = doc_starts(doc_lengths, spots.reshape(-1)).reshape(width, rows).astype(jnp.int32)
    tables = (firsts[:, 0], firsts)

    def cut(value, k):
        size = value.shape[1] // width
        return lax.dynamic_slice_in_dim(value, jnp.bitwise_xor(member, k) * size, size, 1)

    ring = [(fold[i], fold[(i + 1) % parts]) for i in range(parts)]

    def spread(rows):
        def block(k):
            return jnp.concatenate([cut(value, k) for value in rows], axis=1)

        given = jnp.stack([block(k) for k in range(1, width, 2)])
        given = swap(given, 1)
        both = []
        for k in range(0, width, 2):
            both.append(jnp.stack([block(k), given[k // 2]]))
        return [swap(value, 2 * t) for t, value in enumerate(both)]

    pairs = spread([packed_key_rows, packed_value_rows])
    queries = spread([packed_query_rows])
    opens = [(low, low + 2) for low in range(0, width, 2)]

    def move(piece):
        return lax.ppermute(piece, "head", ring)

    held = [(low, jnp.concatenate(pairs[low // 2 : high // 2])) for low, high in opens]
    pieces = [(0, low, piece) for low, piece in held]
    held = [(low, move(piece)) for low, piece in held]
    pieces += [(1, low, piece) for low, piece in held]
    held = [
        (low, jnp.concatenate([piece for at, piece in held if low <= at < low + chunk]))
        for low in range(0, width, chunk)
    ]
    for step in range(2, parts):
        held = [(low, move(piece)) for low, piece in held]
        pieces += [(step, low, piece) for low, piece in held]

    attends = functools.partial(attend, place, tables, queries)
    everyone = list(range(width))
    soon = parts // 2
    first = [piece for piece in pieces if piece[0] < soon]
    state = []
    for slots in (everyone[:chunk], everyone[chunk:]):
        state.append((slots[0], *attends(first, None, slots, [], False, parts)))
    late = [piece for piece in pieces if piece[0] >= soon]
    if docs > width:
        over = [(i, i + width) for i in range(docs - width)]
        far = [(step, low, lax.ppermute(piece, "doc", over)) for step, low, piece in pieces]
        state = [(0, *attends(far, None, everyone, state, False, parts, back=1))]
    near = [piece for piece in late if piece[1] < chunk]
    state = [(0, *attends(near, 0, everyone, state, False, parts))]
    results = {}
    for slots in (everyone[-2:], everyone[:-2]):
        rest = [piece for piece in late if piece[1] >= chunk]
        outs = attends(rest, 1, slots, state, True, parts)
        for slot, out in zip(slots, outs):
            results[slot] = swap(out, slot)
    return collect(place, [results[k] for k in range(width)])


def solution(mesh):
    in_specs = (P(("doc", "head"), None), P(("doc", "head"), None), P(("doc", "head"), None), P())
    out_specs = P(("doc", "head"), None)

    return jax.shard_map(
        on_device, mesh=mesh, in_specs=in_specs, out_specs=out_specs, check_vma=False
    )
```
